512 devices in a mesh: groups: 2 (over y), rows: 64 (over z, core), cols: 4 (over x).
Axes of the slice: x: 4, y: 2, z: 32, core: 2. Of those that a mesh axis runs over, the one named last changes fastest.
The devices are a block of a 4x8x32 slice.
Arguments:
- alignment_features: float32 [2048, 32, 64], P(('groups', 'rows'), 'cols'), parts along dimension 0, may hold values from -6 to 6
- affine_factor: float32 [64], replicated, may hold values from 0.25 to 1.75
- affine_offset: float32 [64], replicated, may hold values from -3 to 3
- first_projector: bfloat16 [64, 32], replicated, may hold values from -0.75 to 0.75
- second_projector: bfloat16 [64, 32], replicated, may hold values from -0.75 to 0.75
- final_projector: bfloat16 [1024, 128], replicated, may hold values from -0.75 to 0.75
- additive_term: float32 [128], replicated, may hold values from -3 to 3
- adjoint_update: bfloat16 [2048, 1024, 128], P(('groups', 'rows'), 'cols'), parts along dimension 0, may hold values from -6 to 6
Outputs:
- residue_update: bfloat16 [2048, 1024, 128], P(('groups', 'rows'), 'cols'), parts along dimension 0
- alignment_slope: float32 [2048, 32, 64], P(('groups', 'rows'), 'cols'), parts along dimension 0
- final_projector_slope: float32 [2048, 128], P(('groups', 'rows', 'cols')), parts along dimension 0
- first_projector_slope: float32 [128, 32], P('groups'), parts along dimension 0
- second_projector_slope: float32 [128, 32], P('groups'), parts along dimension 0
The draws below stay inside these ranges and needn't reach their ends.
There are 2 independent parts, one for each index of `groups`. The reference program is written for one: setup_inputs(seed, part) draws one part's arguments, and reference() takes and returns one part's arrays. A program takes and returns all parts, laid end to end along the dimension named above; an argument that names none is the same for every part. Nothing has to cross between parts.
All inputs are finite; a program needn't handle non-finite values.
Results may differ from the reference program's by a relative error of at most 0.0061.
Values may be sent and summed in bfloat16 or wider, within the bound.
A program may use at most 64 MiB of HBM per device.

```python
import jax
import jax.numpy as jnp
from jax import lax

ALIGNMENT_DEPTH = 64
PROJECTION_WIDTH = 32
FEATURE_DEPTH = 128
ALIGNMENT_ROWS = 32
RESIDUES_EACH = 16
WINDOW_RESIDUES = 1024


def levels(rng, shape, pieces, smallest, high):
    factor_of, own = 1.0, jax.random.fold_in(rng, 6)
    for axis_at, parts in pieces:
        draws = jnp.exp(jax.random.uniform(jax.random.fold_in(own, axis_at), (parts,), jnp.float32, smallest / len(pieces), high / len(pieces)))
        factor_of = factor_of * jnp.repeat(draws, shape[axis_at] // parts).reshape([-1 if axis == axis_at else 1 for axis in range(len(shape))])
    return factor_of


def bell_draw(key, extent, scale, bound, pieces=(), held_as=jnp.bfloat16):
    entries = scale * jax.random.normal(key, extent, jnp.float32)
    if pieces:
        entries = entries * levels(key, extent, pieces, -0.22, 0.18)
    return jnp.clip(entries, -bound, bound).astype(held_as)


def setup_inputs(seed: int = 0, part: int = 0) -> dict:
    arg_keys = jax.random.split(jax.random.key(seed), 9)
    own_keys = jax.random.split(jax.random.fold_in(arg_keys[8], part), 9)
    alignment_features = bell_draw(own_keys[0], (WINDOW_RESIDUES, ALIGNMENT_ROWS, ALIGNMENT_DEPTH), 1.0, 6.0, ((0, 64), (1, 4)), jnp.float32)
    affine_factor = jnp.clip(1.0 + 0.15 * jax.random.normal(arg_keys[1], (ALIGNMENT_DEPTH,), jnp.float32), 0.25, 1.75)
    affine_offset = bell_draw(arg_keys[2], (ALIGNMENT_DEPTH,), 0.5, 3.0, (), jnp.float32)
    first_projector = bell_draw(arg_keys[3], (ALIGNMENT_DEPTH, PROJECTION_WIDTH), ALIGNMENT_DEPTH ** -0.5, 0.75)
    second_projector = bell_draw(arg_keys[4], (ALIGNMENT_DEPTH, PROJECTION_WIDTH), ALIGNMENT_DEPTH ** -0.5, 0.75)
    final_projector = bell_draw(arg_keys[5], (PROJECTION_WIDTH * PROJECTION_WIDTH, FEATURE_DEPTH), (PROJECTION_WIDTH * 2) ** -0.5, 0.75)
    additive_term = bell_draw(arg_keys[6], (FEATURE_DEPTH,), 0.5, 3.0, (), jnp.float32)
    adjoint_update = bell_draw(own_keys[7], (WINDOW_RESIDUES, WINDOW_RESIDUES, FEATURE_DEPTH), 1.0, 6.0, ((0, 64), (1, 4)))
    return dict(alignment_features=alignment_features, affine_factor=affine_factor, affine_offset=affine_offset, first_projector=first_projector, second_projector=second_projector, final_projector=final_projector, additive_term=additive_term, adjoint_update=adjoint_update)


def layernorm_parts(alignment_features, affine_factor, affine_offset):
    centered_alignment = alignment_features - lax.optimization_barrier(jnp.mean(alignment_features, axis=-1, keepdims=True))
    reciprocal_spread = lax.rsqrt(lax.optimization_barrier(jnp.mean(centered_alignment * centered_alignment, axis=-1, keepdims=True)) + 1e-05)
    zscored_alignment = centered_alignment * reciprocal_spread
    return (zscored_alignment, reciprocal_spread, (zscored_alignment * affine_factor + affine_offset).astype(jnp.bfloat16))

def reference(alignment_features, affine_factor, affine_offset, first_projector, second_projector, final_projector, additive_term, adjoint_update):
    zscored_alignment, reciprocal_spread, unit_alignment = layernorm_parts(alignment_features, affine_factor, affine_offset)
    first_factor = jnp.dot(unit_alignment, first_projector, preferred_element_type=jnp.float32).astype(jnp.bfloat16)
    second_factor = jnp.dot(unit_alignment, second_projector, preferred_element_type=jnp.float32).astype(jnp.bfloat16)
    multiplier = 1.0 / ALIGNMENT_ROWS
    right_wide = second_factor.astype(jnp.float32)
    tile_list = WINDOW_RESIDUES // RESIDUES_EACH
    first_tile_list = first_factor.reshape(tile_list, RESIDUES_EACH, ALIGNMENT_ROWS, PROJECTION_WIDTH)
    cot_blocks = adjoint_update.reshape(tile_list, RESIDUES_EACH, WINDOW_RESIDUES, FEATURE_DEPTH)

    def step(carry, inputs):
        right_acc, out_acc = carry
        left_part, cot_part = inputs
        outer = (jnp.einsum('isc,jsd->ijcd', left_part.astype(jnp.float32), right_wide) * multiplier).astype(jnp.bfloat16)
        flat = outer.reshape(RESIDUES_EACH * WINDOW_RESIDUES, PROJECTION_WIDTH * PROJECTION_WIDTH)
        cot_flat = cot_part.reshape(RESIDUES_EACH * WINDOW_RESIDUES, FEATURE_DEPTH)
        update = (jnp.dot(flat, final_projector, preferred_element_type=jnp.float32) + additive_term).astype(jnp.bfloat16)
        outer_grad = jnp.dot(cot_flat, final_projector.T, preferred_element_type=jnp.float32).astype(jnp.bfloat16)
        outer_grad = outer_grad.reshape(RESIDUES_EACH, WINDOW_RESIDUES, PROJECTION_WIDTH, PROJECTION_WIDTH).astype(jnp.float32)
        out_acc = out_acc + jnp.dot(flat.T, cot_flat, preferred_element_type=jnp.float32)
        first_adjoint = jnp.einsum('ijcd,jsd->isc', outer_grad, right_wide) * multiplier
        right_acc = right_acc + jnp.einsum('ijcd,isc->jsd', outer_grad, left_part.astype(jnp.float32)) * multiplier
        return ((right_acc, out_acc), (update.reshape(RESIDUES_EACH, WINDOW_RESIDUES, FEATURE_DEPTH), first_adjoint))
    beginning_position = (jnp.zeros((WINDOW_RESIDUES, ALIGNMENT_ROWS, PROJECTION_WIDTH), jnp.float32), jnp.zeros((PROJECTION_WIDTH * PROJECTION_WIDTH, FEATURE_DEPTH), jnp.float32))
    (right_back, final_projector_slope), (updates, first_adjoint_list) = lax.scan(step, beginning_position, (first_tile_list, cot_blocks))
    residue_update = updates.reshape(WINDOW_RESIDUES, WINDOW_RESIDUES, FEATURE_DEPTH)
    first_adjoint = first_adjoint_list.reshape(WINDOW_RESIDUES, ALIGNMENT_ROWS, PROJECTION_WIDTH)
    unit_broadcast = unit_alignment.astype(jnp.float32)
    high = lax.Precision.HIGHEST
    first_projector_slope = jnp.einsum('tsk,tsc->kc', unit_broadcast, first_adjoint, precision=high)
    second_projector_slope = jnp.einsum('tsk,tsc->kc', unit_broadcast, right_back, precision=high)
    unit_adjoint = jnp.einsum('tsc,kc->tsk', first_adjoint, first_projector.astype(jnp.float32), precision=high)
    unit_adjoint = unit_adjoint + jnp.einsum('tsc,kc->tsk', right_back, second_projector.astype(jnp.float32), precision=high)
    scaled_alignment = unit_adjoint * affine_factor
    alignment_slope = reciprocal_spread * (scaled_alignment - lax.optimization_barrier(jnp.mean(scaled_alignment, axis=-1, keepdims=True)) - zscored_alignment * lax.optimization_barrier(jnp.mean(scaled_alignment * zscored_alignment, axis=-1, keepdims=True)))
    return (residue_update, alignment_slope, final_projector_slope, first_projector_slope, second_projector_slope)
```

```python
import functools

import jax
import jax.numpy as jnp
from jax import lax
from jax.experimental import pallas as pl
from jax.experimental.pallas import tpu as pltpu
from jax.sharding import PartitionSpec as P

F32 = jnp.float32
BF16 = jnp.bfloat16
NEAR = 4
CORES = 2
SEMS = 96


def iota(shape, dim):
    return lax.broadcasted_iota(jnp.int32, shape, dim)


def nn(a, b):
    return jnp.dot(a, b, preferred_element_type=F32)


def nt(a, b):
    return lax.dot_general(a, b, (((1,), (1,)), ((), ())), preferred_element_type=F32)


def tn(a, b):
    return lax.dot_general(a, b, (((0,), (0,)), ((), ())), preferred_element_type=F32)


def two_part(form, a, b):
    high = a.astype(BF16)
    low = (a - high.astype(F32)).astype(BF16)
    return form(high, b) + form(low, b)


def two_part_right(form, a, b):
    high = b.astype(BF16)
    low = (b - high.astype(F32)).astype(BF16)
    return form(a, high) + form(a, low)


def kernel(
    X, Z, feat, gain, offset, p1, p2, w, bias, cot,
    out, slope, wslope, slope1, slope2,
    wf, wb, lf, lp2, lpt2, ring_r, r_all, rt, t_all, q_all,
    rb_bf, rb_own, rb_d, rb_n, rb_o, rb_r, rb_x, rb_q, ru_s, ru_r, rd_s, rd_r,
    lb_acc, lb, lb_r, s_all, s_d, s_x, s_xr, s_n, s_nr, s_g, s_row,
    v_s, v_rs, v_n, v_nr, v_g, v_f, send_sem, recv_sem,
):
    ring = Z // NEAR
    mem = Z // X // NEAR
    tok = feat.shape[0]
    pairs = tok // 2
    s8 = feat.shape[1]
    width = w.shape[0] // p1.shape[1]
    lanes = width * s8
    xi = lax.axis_index("cols")
    row = lax.axis_index("rows")
    z, core = row // CORES, row % CORES
    a, m = z % NEAR, z // NEAR
    scale = 1.0 / (s8 * X)

    def at(dx=0, dz=0, other=None):
        k = core if other is None else other
        return {"rows": ((z + dz + Z) % Z) * CORES + k, "cols": (xi + dx) % X}

    used = [0]

    def send(src, dst, device):
        k = used[0]
        used[0] += 1
        copy = pltpu.make_async_remote_copy(
            src_ref=src, dst_ref=dst, send_sem=send_sem.at[k], recv_sem=recv_sem.at[k],
            device_id=device, device_id_type=pl.DeviceIdType.MESH,
        )
        copy.start()
        return copy

    started = []

    def go(src, dst, device):
        copy = send(src, dst, device)
        started.append(copy)
        return copy

    level = CORES * X
    here = xi * CORES + core

    def peer(o):
        there = (here + o) % level
        return there, {"rows": z * CORES + there % CORES, "cols": there // CORES}

    steps = (1, -1, 2, -2, NEAR, -NEAR)
    barrier = pltpu.get_barrier_semaphore()
    for o in range(1, level):
        pl.semaphore_signal(barrier, inc=1, device_id=peer(o)[1], device_id_type=pl.DeviceIdType.MESH)
    for dz in steps:
        pl.semaphore_signal(barrier, inc=1, device_id=at(dz=dz), device_id_type=pl.DeviceIdType.MESH)

    f = feat[...]
    centred = f - jnp.mean(f, axis=-1, keepdims=True)
    rs = lax.rsqrt(jnp.mean(centred * centred, axis=-1, keepdims=True) + 1e-05)
    xhat = centred * rs
    normed = xhat * gain[...][None] + offset[...][None]
    depth = f.shape[2]
    split = normed.reshape(pairs, 2, s8, depth)
    even = split[:, 0].reshape(pairs * s8, depth).astype(BF16)
    odd = split[:, 1].reshape(pairs * s8, depth).astype(BF16)
    nb = normed.reshape(tok * s8, depth).astype(BF16)

    rep = (iota((width, lanes), 1) // s8 == iota((width, lanes), 0)).astype(BF16)
    p2r = nn(p2[...], rep).astype(BF16)
    half = 2 * 2 * width
    col = iota((width, half), 1)
    same = col % width == iota((width, half), 0)
    p1e = nn(p1[...], (same & ((col // width) % 2 == 0)).astype(BF16)).astype(BF16)
    p1o = nn(p1[...], (same & ((col // width) % 2 == 1)).astype(BF16)).astype(BF16)
    pick = iota((tok, s8, lanes), 1) == iota((tok, s8, lanes), 2) % s8

    right = nn(nb, p2r).reshape(tok, s8, lanes)
    ring_r[m] = jnp.sum(jnp.where(pick, right, 0.0), axis=1).astype(BF16)
    left = (nn(even, p1e) + nn(odd, p1o)).astype(BF16).astype(F32)
    lf[:, xi] = left.reshape(pairs, s8, half)

    wf[...] = w[...].astype(F32)
    wb[...] = jnp.zeros_like(wb)

    def spread(g, _):
        for d2 in range(2):
            piece = wf[pl.ds(2 * g + d2, width, stride=width), :].astype(BF16)
            for i in range(2):
                at_row = (d2 * 2 + i) * width
                wb[g, at_row : at_row + width, i * 128 : (i + 1) * 128] = piece
        return 0

    lax.fori_loop(0, width // 2, spread, 0)
    pl.semaphore_wait(barrier, level - 1 + len(steps))

    def ring_up(buf, t):
        q = (m - t + 1 + ring) % ring
        return go(buf.at[q], buf.at[q], at(dz=NEAR))

    def ring_down(buf, t):
        q = (m + t - 1) % ring
        return go(buf.at[q], buf.at[q], at(dz=-NEAR))

    ups, downs = ring // 2, ring // 2 - 1

    lefts = [go(lf.at[:, xi], lf.at[:, xi], at(dx=dx)) for dx in range(1, X)]
    up, down = ring_up(ring_r, 1), ring_down(ring_r, 1)
    for copy in lefts:
        copy.wait_recv()

    lane = iota((pairs * X, s8, half), 2)
    lfull = lf[...].reshape(pairs * X, s8, half)
    zero = jnp.zeros_like(lfull)
    both = jnp.concatenate(
        [jnp.where(lane < half // 2, lfull, zero), jnp.where(lane >= half // 2, lfull, zero)], axis=1
    )
    lp2[...] = both.reshape(pairs * X * s8 * 2, half).astype(BF16)
    er, ec = iota((half, half), 0), iota((half, half), 1)
    kept = (er // width) * width + (er % ring) * NEAR + (er % width) // ring
    lpt2[...] = nt((kept == ec).astype(BF16), lp2[...]).astype(BF16)

    def make_t(g, _):
        piece = nn(lp2[...], wb[g]).astype(BF16).reshape(pairs, X, 2 * s8, 256)
        t_all[:, :, pl.ds(pl.multiple_of(g * 2 * s8, 2 * s8), 2 * s8), :] = piece
        return 0

    lax.fori_loop(0, width // 2, make_t, 0)

    up.wait_recv()
    up2 = ring_up(ring_r, 2)
    down.wait_recv()
    down2 = ring_down(ring_r, 2)

    def pair_of(p):
        return jnp.concatenate([cot[2 * p], cot[2 * p + 1]], axis=-1)

    def make_rb(k, _):
        total = nt(pair_of(0), t_all[0, k])
        for p in range(1, pairs):
            total = total + nt(pair_of(p), t_all[p, k])
        total = (total * scale).reshape(mem, NEAR, CORES, tok, lanes)
        rb_bf[k] = total.astype(BF16)
        rb_own[k] = total
        return 0

    lax.fori_loop(0, X, make_rb, 0)
    rbd = go(rb_bf.at[:, :, :, 1 - core], rb_d, at(other=1 - core))

    up2.wait_recv()
    up3 = ring_up(ring_r, 3)
    down2.wait_recv()
    down3 = ring_down(ring_r, 3)

    rbd.wait_recv()
    for k in range(NEAR):
        piece = rb_own[:, :, k, core] + rb_d[:, :, k].astype(F32)
        rb_n[k] = piece.astype(BF16)
    rb_o[...] = rb_own[:, :, a, core] + rb_d[:, :, a].astype(F32)
    hx = X // 2
    rbn = [
        go(rb_n.at[(a + 1) % NEAR], rb_r.at[0], at(dz=1)),
        go(rb_n.at[(a + 3) % NEAR], rb_r.at[1], at(dz=-1)),
        go(rb_n.at[(a + 2) % NEAR, 0:hx], rb_r.at[2, 0:hx], at(dz=2)),
        go(rb_n.at[(a + 2) % NEAR, hx:X], rb_r.at[2, hx:X], at(dz=-2)),
    ]

    up3.wait_recv()
    up4 = ring_up(ring_r, 4)

    for copy in rbn:
        copy.wait_recv()
    rb_x[...] = (
        rb_o[...] + rb_r[0].astype(F32) + rb_r[1].astype(F32) + rb_r[2].astype(F32)
    ).astype(BF16)
    rb_q[pl.ds(xi * mem, mem)] = rb_x[xi]
    rbx = [
        go(rb_x.at[(xi + dx) % X], rb_q.at[pl.ds(xi * mem, mem)], at(dx=dx)) for dx in range(1, X)
    ]

    up4.wait_recv()
    down3.wait_recv()
    r_all[xi, :, a, core] = ring_r[pl.ds(xi * mem, mem)]
    rx = [
        go(ring_r.at[pl.ds(((xi + dx) % X) * mem, mem)], r_all.at[xi, :, a, core], at(dx=dx))
        for dx in range(1, X)
    ]

    for copy in rbx:
        copy.wait_recv()

    def rb_up(t):
        q = (m + ups + 1 - t) % ring
        value = rb_q[q].astype(F32)
        if t > 1:
            value = value + ru_r[t - 2].astype(F32)
        ru_s[t - 1] = value.astype(BF16)
        return go(ru_s.at[t - 1], ru_r.at[t - 1], at(dz=NEAR))

    def rb_down(t):
        q = (m - downs - 1 + t + ring) % ring
        value = rb_q[q].astype(F32)
        if t > 1:
            value = value + rd_r[t - 2].astype(F32)
        rd_s[t - 1] = value.astype(BF16)
        return go(rd_s.at[t - 1], rd_r.at[t - 1], at(dz=-NEAR))

    bu, bd = rb_up(1), rb_down(1)

    for copy in rx:
        copy.wait_recv()
    rn = [
        go(r_all.at[:, :, a, core], r_all.at[:, :, a, core], at(dz=1)),
        go(r_all.at[:, :, a, core], r_all.at[:, :, a, core], at(dz=-1)),
        go(r_all.at[0:hx, :, a, core], r_all.at[0:hx, :, a, core], at(dz=2)),
        go(r_all.at[hx:X, :, a, core], r_all.at[hx:X, :, a, core], at(dz=-2)),
    ]
    partner = at(other=1 - core)

    def to_partner(k):
        return go(r_all.at[:, :, k, core], r_all.at[:, :, k, core], partner)

    cores = [to_partner(a)]

    bu.wait_recv()
    bu = rb_up(2)
    bd.wait_recv()
    bd = rb_down(2)

    rn[0].wait_recv()
    cores.append(to_partner((a + 3) % NEAR))
    rn[1].wait_recv()
    cores.append(to_partner((a + 1) % NEAR))
    rn[2].wait_recv()
    rn[3].wait_recv()
    cores.append(to_partner((a + 2) % NEAR))
    for copy in cores:
        copy.wait_recv()

    block = mem * NEAR * CORES * tok

    def turn(k, _):
        rt[k] = r_all[k].reshape(block, lanes).T
        return 0

    lax.fori_loop(0, X, turn, 0)

    def make_q(p, _):
        pair = pair_of(p)
        for k in range(X):
            q_all[p, k] = nn(rt[k], pair).astype(BF16)
        return 0

    lax.fori_loop(0, pairs, make_q, 0)

    lb_acc[...] = jnp.zeros_like(lb_acc)

    def make_s(g, _):
        for u in range(2):
            at_row = pl.multiple_of((2 * g + u) * 2 * s8, 2 * s8)
            piece = q_all[:, :, pl.ds(at_row, 2 * s8), :].reshape(pairs * X * 2 * s8, 256)
            lb_acc[...] += nt(piece, wb[2 * g + u])
            found = nn(lpt2[...], piece) * scale
            for d2 in range(2):
                top = d2 * 2 * width
                s_all[g, :, (2 * u + d2) * 128 : (2 * u + d2 + 1) * 128] = (
                    found[top : top + width, 0:128] + found[top + width : top + 2 * width, 128:256]
                )
        return 0

    lax.fori_loop(0, width // 4, make_s, 0)
    sd = go(s_all.at[pl.ds((1 - core) * X, X)], s_d, partner)
    acc = lb_acc[...].reshape(pairs * X, 2, s8, half)
    lb[...] = (jnp.where(lane < half // 2, acc[:, 0], acc[:, 1]) * scale).reshape(pairs, X, s8, half)
    lbx = [go(lb.at[:, (xi + dx) % X], lb_r.at[dx - 1], at(dx=dx)) for dx in range(1, X)]

    bu.wait_recv()
    bu = rb_up(3)
    bd.wait_recv()
    bd = rb_down(3)

    sd.wait_recv()
    s_x[...] = (s_all[pl.ds(core * X, X)] + s_d[...]).astype(BF16)
    sx = [go(s_x.at[(xi + dx) % X], s_xr.at[dx - 1], at(dx=dx)) for dx in range(1, X)]

    def make_update(p, _):
        total = nn(r_all[0].reshape(block, lanes), t_all[p, 0])
        for k in range(1, X):
            total = total + nn(r_all[k].reshape(block, lanes), t_all[p, k])
        total = total * scale
        out[2 * p] = (total[:, 0:128] + bias[...]).astype(BF16)
        out[2 * p + 1] = (total[:, 128:256] + bias[...]).astype(BF16)
        return 0

    lax.fori_loop(0, pairs // 2, make_update, 0)

    for copy in lbx:
        copy.wait_recv()
    lsum = (lb[:, xi] + lb_r[0] + lb_r[1] + lb_r[2]).reshape(pairs * s8, half)

    for copy in sx:
        copy.wait_recv()
    stot = s_x[xi].astype(F32)
    for k in range(X - 1):
        stot = stot + s_xr[k].astype(F32)
    s_n[...] = stot.reshape(NEAR, ring, stot.shape[1])
    sn = [
        go(s_n.at[(a + 1) % NEAR], s_nr.at[0], at(dz=1)),
        go(s_n.at[(a + 3) % NEAR], s_nr.at[1], at(dz=-1)),
        go(s_n.at[(a + 2) % NEAR], s_nr.at[2], at(dz=2)),
    ]

    bu.wait_recv()
    bu = rb_up(4)
    lax.fori_loop(pairs // 2, pairs, make_update, 0)

    for copy in sn:
        copy.wait_recv()
    tile = s_n[a] + s_nr[0] + s_nr[1] + s_nr[2]
    s_g[m] = jnp.concatenate([tile[:, 0:256], tile[:, 256:512]], axis=0).astype(BF16)
    su, sdn = ring_up(s_g, 1), ring_down(s_g, 1)

    bu.wait_recv()
    bd.wait_recv()
    rb = rb_q[m].astype(F32) + ru_r[ups - 1].astype(F32) + rd_r[downs - 1].astype(F32)
    wide = jnp.where(pick, rb.reshape(tok, 1, lanes), 0.0).reshape(tok * s8, lanes)

    f1 = two_part_right(tn, even, lsum)
    f2 = two_part_right(tn, odd, lsum)
    ftot = jnp.where((iota(f1.shape, 1) // width) % 2 == 0, f1, f2)
    fold1 = (er % width == ec).astype(BF16)
    g2 = two_part_right(tn, nb, wide)
    fold2 = (iota((lanes, half), 0) // s8 + width == iota((lanes, half), 1)).astype(BF16)
    vtot = two_part(nn, ftot, fold1) + two_part(nn, g2, fold2)
    v_s[...] = vtot.reshape(level, depth // level, half)
    vrs = []
    for o in range(1, level):
        there, device = peer(o)
        vrs.append(go(v_s.at[there], v_rs.at[o - 1], device))

    from_right = two_part(nt, wide, p2r)
    from_even = two_part(nt, lsum, p1e).reshape(pairs, 1, s8, depth)
    from_odd = two_part(nt, lsum, p1o).reshape(pairs, 1, s8, depth)
    from_left = jnp.concatenate([from_even, from_odd], axis=1).reshape(tok, s8, depth)
    scaled = (from_right.reshape(tok, s8, depth) + from_left) * gain[...][None]
    slope[...] = rs * (
        scaled
        - jnp.mean(scaled, axis=-1, keepdims=True)
        - xhat * jnp.mean(scaled * xhat, axis=-1, keepdims=True)
    )

    for copy in vrs:
        copy.wait_recv()
    vsum = v_s[here]
    for k in range(level - 1):
        vsum = vsum + v_rs[k]
    v_n[...] = vsum
    vn = [go(v_n, v_nr.at[k], at(dz=dz)) for k, dz in enumerate((1, -1, 2))]
    su.wait_recv()
    su = ring_up(s_g, 2)
    sdn.wait_recv()
    sdn = ring_down(s_g, 2)
    for copy in vn:
        copy.wait_recv()
    v_g[m] = v_n[...] + v_nr[0] + v_nr[1] + v_nr[2]
    vu, vd = ring_up(v_g, 1), ring_down(v_g, 1)
    for t in range(3, ups + 1):
        su.wait_recv()
        su = ring_up(s_g, t)
        if t <= downs:
            sdn.wait_recv()
            sdn = ring_down(s_g, t)
        vu.wait_recv()
        vu = ring_up(v_g, t - 1)
        vd.wait_recv()
        vd = ring_down(v_g, t - 1) if t - 1 <= downs else None
    su.wait_recv()
    if downs > 2:
        sdn.wait_recv()
    vu.wait_recv()
    vu = ring_up(v_g, ups)
    stile = s_g[0].astype(F32)
    for k in range(1, ring):
        stile = stile + s_g[k].astype(F32)
    s_row[...] = stile
    for h in range(2):
        line = s_row[pl.ds(m + h * ring, 1), :]
        wslope[2 * h : 2 * h + 1, :] = line[:, 0:128]
        wslope[2 * h + 1 : 2 * h + 2, :] = line[:, 128:256]
    vu.wait_recv()
    if vd is not None:
        vd.wait_recv()
    vtile = v_g[0]
    for k in range(1, ring):
        vtile = vtile + v_g[k]
    v_f[here] = vtile
    vag = [go(v_f.at[here], v_f.at[here], peer(o)[1]) for o in range(1, level)]
    for copy in vag:
        copy.wait_recv()
    vfull = v_f[...].reshape(depth, half)
    slope1[...] = vfull[:, 0:width]
    slope2[...] = vfull[:, width : 2 * width]

    for copy in started:
        copy.wait_send()


def solution(mesh):
    X, Z = mesh.shape["cols"], mesh.shape["rows"] // CORES

    def local(feat, gain, offset, p1, p2, w, bias, cot):
        tok, s8, depth = feat.shape
        width = p1.shape[1]
        pair_ch = w.shape[1]
        block = cot.shape[1]
        ring, mem, pairs = Z // NEAR, Z // X // NEAR, tok // 2
        lanes, half, seqs = width * s8, 4 * width, s8 * X
        level = CORES * X
        v = pltpu.VMEM
        scratch = [
            v(w.shape, F32),
            v((width // 2, half, 2 * pair_ch), BF16),
            v((pairs, X, s8, half), F32),
            v((pairs * seqs * 2, half), BF16),
            v((half, pairs * seqs * 2), BF16),
            v((ring, tok, lanes), BF16),
            v((X, mem, NEAR, CORES, tok, lanes), BF16),
            v((X, lanes, block), BF16),
            v((pairs, X, lanes, 2 * pair_ch), BF16),
            v((pairs, X, lanes, 2 * pair_ch), BF16),
            v((X, mem, NEAR, CORES, tok, lanes), BF16),
            v((X, mem, NEAR, CORES, tok, lanes), F32),
            v((X, mem, NEAR, tok, lanes), BF16),
            v((NEAR, X, mem, tok, lanes), BF16),
            v((X, mem, tok, lanes), F32),
            v((NEAR - 1, X, mem, tok, lanes), BF16),
            v((X, mem, tok, lanes), BF16),
            v((ring, tok, lanes), BF16),
            v((ring // 2, tok, lanes), BF16),
            v((ring // 2, tok, lanes), BF16),
            v((ring // 2, tok, lanes), BF16),
            v((ring // 2, tok, lanes), BF16),
            v((pairs * seqs * 2, half), F32),
            v((pairs, X, s8, half), F32),
            v((X - 1, pairs, s8, half), F32),
            v((CORES * X, width, width // level * pair_ch), F32),
            v((X, width, width // level * pair_ch), F32),
            v((X, width, width // level * pair_ch), BF16),
            v((X - 1, width, width // level * pair_ch), BF16),
            v((NEAR, ring, width // level * pair_ch), F32),
            v((NEAR - 1, ring, width // level * pair_ch), F32),
            v((ring, 2 * ring, 2 * pair_ch), BF16),
            v((2 * ring, 2 * pair_ch), F32),
            v((level, depth // level, half), F32),
            v((level - 1, depth // level, half), F32),
            v((depth // level, half), F32),
            v((NEAR - 1, depth // level, half), F32),
            v((ring, depth // level, half), F32),
            v((level, depth // level, half), F32),
            pltpu.SemaphoreType.DMA((SEMS,)),
            pltpu.SemaphoreType.DMA((SEMS,)),
        ]
        whole = pl.BlockSpec(memory_space=pltpu.VMEM)
        shape = jax.ShapeDtypeStruct
        return pl.pallas_call(
            functools.partial(kernel, X, Z),
            out_shape=(
                shape(cot.shape, BF16),
                shape(feat.shape, F32),
                shape((w.shape[0] // (Z * level), pair_ch), F32),
                shape((depth, width), F32),
                shape((depth, width), F32),
            ),
            in_specs=[whole] * 8,
            out_specs=(whole,) * 5,
            scratch_shapes=scratch,
            compiler_params=pltpu.CompilerParams(collective_id=0, has_side_effects=True),
            name="outer_mean",
        )(feat, gain.reshape(1, -1), offset.reshape(1, -1), p1, p2, w, bias.reshape(1, -1), cot)

    tokens = P(("groups", "rows"), "cols", None)
    return jax.shard_map(
        local,
        mesh=mesh,
        in_specs=(tokens, P(), P(), P(), P(), P(), P(), tokens),
        out_specs=(tokens, tokens, P(("groups", "rows", "cols"), None), P("groups", None), P("groups", None)),
        check_vma=False,
    )
```

```python
import functools

import jax
import jax.numpy as jnp
from jax import lax
from jax.experimental import pallas as pl
from jax.experimental.pallas import tpu as pltpu
from jax.sharding import PartitionSpec as P

F32 = jnp.float32
BF16 = jnp.bfloat16
NEAR = 4
CORES = 2
SEMS = 96
VMEM_BYTES = 66 * 1000 * 1000


def iota(shape, dim):
    return lax.broadcasted_iota(jnp.int32, shape, dim)


def nn(a, b):
    return jnp.dot(a, b, preferred_element_type=F32)


def nt(a, b):
    return lax.dot_general(a, b, (((1,), (1,)), ((), ())), preferred_element_type=F32)


def tn(a, b):
    return lax.dot_general(a, b, (((0,), (0,)), ((), ())), preferred_element_type=F32)


def two_part(form, a, b):
    high = a.astype(BF16)
    low = (a - high.astype(F32)).astype(BF16)
    return form(high, b) + form(low, b)


def kernel(
    X, Z, feat_in, gain_in, offset_in, p1_in, p2_in, w_in, bias_in, cot_in,
    out_away, slope, wslope, slope1, slope2,
    out, feat, gain, offset, p1, p2, w, bias, cot, wf, wb, lf, lp2, lpt2, ring_r, r_all, rt, t_all, q_all,
    rb_bf, rb_own, rb_d, rb_n, rb_o, rb_r, rb_x, rb_q, rb_f,
    lb_acc, lb, lb_r, s_all, s_rs, s_n, s_nr, s_f, s_fr,
    v_s, v_rs, v_n, v_nr, v_t, v_fr, v_f, send_sem, recv_sem, load_sem,
):
    ring = Z // NEAR
    mem = Z // X // NEAR
    tok = feat.shape[0]
    pairs = tok // 2
    s8 = feat.shape[1]
    width = p1.shape[0]
    lanes = width * s8
    xi = lax.axis_index("cols")
    row = lax.axis_index("rows")
    z, core = row // CORES, row % CORES
    a, m = z % NEAR, z // NEAR
    scale = 1.0 / (s8 * X)

    def at(dx=0, dz=0, other=None):
        k = core if other is None else other
        return {"rows": ((z + dz + Z) % Z) * CORES + k, "cols": (xi + dx) % X}

    used = [0]

    def send(src, dst, device):
        k = used[0]
        used[0] += 1
        copy = pltpu.make_async_remote_copy(
            src_ref=src, dst_ref=dst, send_sem=send_sem.at[k], recv_sem=recv_sem.at[k],
            device_id=device, device_id_type=pl.DeviceIdType.MESH,
        )
        copy.start()
        return copy

    started = []

    def go(src, dst, device):
        copy = send(src, dst, device)
        started.append(copy)
        return copy

    level = CORES * X
    here = xi * CORES + core

    def peer(o):
        there = (here + o) % level
        return there, {"rows": z * CORES + there % CORES, "cols": there // CORES}

    sources = (feat_in, gain_in, offset_in, p2_in, p1_in, w_in, bias_in, cot_in)
    targets = (feat, gain, offset, p2, p1, w, bias, cot)
    loads = [
        pltpu.make_async_copy(source, target, load_sem.at[k])
        for k, (source, target) in enumerate(zip(sources, targets))
    ]
    for copy in loads:
        copy.start()
    steps = (1, -1, 2, -2, NEAR, -NEAR)
    barrier = pltpu.get_barrier_semaphore()
    for o in range(1, level):
        pl.semaphore_signal(barrier, inc=1, device_id=peer(o)[1], device_id_type=pl.DeviceIdType.MESH)
    for dz in steps:
        pl.semaphore_signal(barrier, inc=1, device_id=at(dz=dz), device_id_type=pl.DeviceIdType.MESH)

    for copy in loads[:5]:
        copy.wait()
    f = feat[...]
    centred = f - jnp.mean(f, axis=-1, keepdims=True)
    rs = lax.rsqrt(jnp.mean(centred * centred, axis=-1, keepdims=True) + 1e-05)
    xhat = centred * rs
    normed = xhat * gain[...][None] + offset[...][None]
    depth = f.shape[2]
    split = normed.reshape(pairs, 2, s8, depth)
    even = split[:, 0].reshape(pairs * s8, depth).astype(BF16)
    odd = split[:, 1].reshape(pairs * s8, depth).astype(BF16)
    nb = normed.reshape(tok * s8, depth).astype(BF16)

    rep = (iota((width, lanes), 1) // s8 == iota((width, lanes), 0)).astype(BF16)
    p2r = tn(p2[...], rep).astype(BF16)
    half = 2 * 2 * width
    col = iota((width, half), 1)
    same = col % width == iota((width, half), 0)
    p1e = tn(p1[...], (same & ((col // width) % 2 == 0)).astype(BF16)).astype(BF16)
    p1o = tn(p1[...], (same & ((col // width) % 2 == 1)).astype(BF16)).astype(BF16)
    pick = iota((tok, s8, lanes), 1) == iota((tok, s8, lanes), 2) % s8

    right = nn(nb, p2r).reshape(tok, s8, lanes)
    ring_r[m] = jnp.sum(jnp.where(pick, right, 0.0), axis=1).astype(BF16)
    left = (nn(even, p1e) + nn(odd, p1o)).astype(BF16).astype(F32)
    lf[:, xi] = left.reshape(pairs, s8, half)

    wb[...] = jnp.zeros_like(wb)
    loads[5].wait()
    wf[...] = w[...].astype(F32)

    def spread(g, _):
        for d2 in range(2):
            piece = wf[pl.ds(2 * g + d2, width, stride=width), :].astype(BF16)
            for i in range(2):
                at_row = (d2 * 2 + i) * width
                wb[g, at_row : at_row + width, i * 128 : (i + 1) * 128] = piece
        return 0

    lax.fori_loop(0, width // 2, spread, 0)
    pl.semaphore_wait(barrier, level - 1 + len(steps))

    def ring_up(buf, t):
        q = (m - t + 1 + ring) % ring
        return go(buf.at[q], buf.at[q], at(dz=NEAR))

    def ring_down(buf, t):
        q = (m + t - 1) % ring
        return go(buf.at[q], buf.at[q], at(dz=-NEAR))

    ups, downs = ring // 2, ring // 2 - 1

    lefts = [go(lf.at[:, xi], lf.at[:, xi], at(dx=dx)) for dx in range(1, X)]
    up, down = ring_up(ring_r, 1), ring_down(ring_r, 1)
    for copy in lefts:
        copy.wait_recv()

    lane = iota((pairs * X, s8, half), 2)
    lfull = lf[...].reshape(pairs * X, s8, half)
    zero = jnp.zeros_like(lfull)
    both = jnp.concatenate(
        [jnp.where(lane < half // 2, lfull, zero), jnp.where(lane >= half // 2, lfull, zero)], axis=1
    )
    lp2[...] = both.reshape(pairs * X * s8 * 2, half).astype(BF16)
    er, ec = iota((half, half), 0), iota((half, half), 1)
    kept = (er // width) * width + (er % ring) * NEAR + (er % width) // ring
    lpt2[...] = nt((kept == ec).astype(BF16), lp2[...]).astype(BF16)

    def make_t(g, _):
        for u in range(2):
            piece = nn(lp2[...], wb[2 * g + u]).astype(BF16).reshape(pairs, X, 2 * s8, 256)
            at_row = pl.multiple_of((2 * g + u) * 2 * s8, 2 * s8)
            t_all[:, :, pl.ds(at_row, 2 * s8), :] = piece
        return 0

    lax.fori_loop(0, width // 8, make_t, 0)

    up.wait_recv()
    up2 = ring_up(ring_r, 2)
    down.wait_recv()
    down2 = ring_down(ring_r, 2)
    lax.fori_loop(width // 8, width // 4, make_t, 0)
    loads[6].wait()
    loads[7].wait()

    def pair_of(p):
        return jnp.concatenate([cot[2 * p], cot[2 * p + 1]], axis=-1)

    def make_rb(k, _):
        total = nt(pair_of(0), t_all[0, k])
        for p in range(1, pairs):
            total = total + nt(pair_of(p), t_all[p, k])
        total = (total * scale).reshape(mem, NEAR, CORES, tok, lanes)
        rb_bf[k] = total.astype(BF16)
        rb_own[k] = total
        return 0

    lax.fori_loop(0, X, make_rb, 0)
    rbd = go(rb_bf.at[:, :, :, 1 - core], rb_d, at(other=1 - core))

    up2.wait_recv()
    up3 = ring_up(ring_r, 3)
    down2.wait_recv()
    down3 = ring_down(ring_r, 3)

    rbd.wait_recv()
    for k in range(NEAR):
        piece = rb_own[:, :, k, core] + rb_d[:, :, k].astype(F32)
        rb_n[k] = piece.astype(BF16)
    hx = X // 2
    rbn = [
        go(rb_n.at[(a + 1) % NEAR], rb_r.at[0], at(dz=1)),
        go(rb_n.at[(a + 3) % NEAR], rb_r.at[1], at(dz=-1)),
        go(rb_n.at[(a + 2) % NEAR, 0:hx], rb_r.at[2, 0:hx], at(dz=2)),
        go(rb_n.at[(a + 2) % NEAR, hx:X], rb_r.at[2, hx:X], at(dz=-2)),
    ]
    rb_o[...] = rb_own[:, :, a, core] + rb_d[:, :, a].astype(F32)

    up3.wait_recv()
    up4 = ring_up(ring_r, 4)

    for copy in rbn:
        copy.wait_recv()
    rb_x[...] = (
        rb_o[...] + rb_r[0].astype(F32) + rb_r[1].astype(F32) + rb_r[2].astype(F32)
    ).astype(BF16)
    rbx = [
        go(rb_x.at[(xi + dx) % X], rb_q.at[pl.ds(xi * mem, mem)], at(dx=dx)) for dx in range(1, X)
    ]
    rb_q[pl.ds(xi * mem, mem)] = rb_x[xi]

    down3.wait_recv()
    up4.wait_recv()
    rx = [
        go(ring_r.at[pl.ds(((xi + dx) % X) * mem, mem)], r_all.at[xi, :, a, core], at(dx=dx))
        for dx in range(1, X)
    ]
    r_all[xi, :, a, core] = ring_r[pl.ds(xi * mem, mem)]
    partner = at(other=1 - core)

    for copy in rx:
        copy.wait_recv()
    rn = [
        go(r_all.at[:, :, a, core], r_all.at[:, :, a, core], at(dz=1)),
        go(r_all.at[:, :, a, core], r_all.at[:, :, a, core], at(dz=-1)),
        go(r_all.at[0:hx, :, a, core], r_all.at[0:hx, :, a, core], at(dz=2)),
        go(r_all.at[hx:X, :, a, core], r_all.at[hx:X, :, a, core], at(dz=-2)),
    ]

    def to_partner(k):
        return go(r_all.at[:, :, k, core], r_all.at[:, :, k, core], partner)

    cores = [to_partner(a)]

    def far(o):
        return (m + o) % ring, at(dz=NEAR * o)

    for copy in rbx:
        copy.wait_recv()
    rbf = []
    for o in range(1, ring):
        there, device = far(o)
        rbf.append(go(rb_q.at[there], rb_f.at[o - 1], device))

    rn[0].wait_recv()
    cores.append(to_partner((a + 3) % NEAR))
    rn[1].wait_recv()
    cores.append(to_partner((a + 1) % NEAR))
    rn[2].wait_recv()
    rn[3].wait_recv()
    cores.append(to_partner((a + 2) % NEAR))
    for copy in cores:
        copy.wait_recv()

    block = mem * NEAR * CORES * tok

    def turn(k, _):
        rt[k] = r_all[k].reshape(block, lanes).T
        return 0

    lax.fori_loop(0, X, turn, 0)

    def make_q(p, _):
        pair = pair_of(p)
        for k in range(X):
            q_all[p, k] = nn(rt[k], pair).astype(BF16)
        return 0

    lax.fori_loop(0, pairs, make_q, 0)

    lb_acc[...] = jnp.zeros_like(lb_acc)

    def of_q(g):
        at_row = pl.multiple_of(g * 2 * s8, 2 * s8)
        return q_all[:, :, pl.ds(at_row, 2 * s8), :].reshape(pairs * X * 2 * s8, 256)

    def make_lb(g, _):
        total = nt(of_q(4 * g), wb[4 * g])
        for u in range(1, 4):
            total = total + nt(of_q(4 * g + u), wb[4 * g + u])
        lb_acc[...] += total
        return 0

    lax.fori_loop(0, width // 8, make_lb, 0)
    acc = lb_acc[...].reshape(pairs * X, 2, s8, half)
    lb[...] = (jnp.where(lane < half // 2, acc[:, 0], acc[:, 1]) * scale).reshape(pairs, X, s8, half)
    lbx = [go(lb.at[:, (xi + dx) % X], lb_r.at[dx - 1], at(dx=dx)) for dx in range(1, X)]

    def make_s(g, _):
        there = (g % X) * CORES + g // X
        for u in range(2):
            found = nn(lpt2[...], of_q(2 * g + u)) * scale
            for d2 in range(2):
                top = d2 * 2 * width
                s_all[there, :, (2 * u + d2) * 128 : (2 * u + d2 + 1) * 128] = (
                    found[top : top + width, 0:128] + found[top + width : top + 2 * width, 128:256]
                ).astype(BF16)
        return 0

    lax.fori_loop(0, width // 4, make_s, 0)
    srs = []
    for o in range(1, level):
        there, device = peer(o)
        srs.append(go(s_all.at[there], s_rs.at[o - 1], device))

    def make_update(p, _):
        total = nn(r_all[0].reshape(block, lanes), t_all[p, 0])
        for k in range(1, X):
            total = total + nn(r_all[k].reshape(block, lanes), t_all[p, k])
        total = total * scale
        out[2 * p] = (total[:, 0:128] + bias[...]).astype(BF16)
        out[2 * p + 1] = (total[:, 128:256] + bias[...]).astype(BF16)
        return 0

    for copy in lbx:
        copy.wait_recv()
    lsum = (lb[:, xi] + lb_r[0] + lb_r[1] + lb_r[2]).reshape(pairs * s8, half)
    f1 = two_part(tn, lsum, even)
    f2 = two_part(tn, lsum, odd)
    left_slope = f1[0:width] + f1[2 * width : 3 * width] + f2[width : 2 * width] + f2[3 * width :]
    lax.fori_loop(0, pairs // 4, make_update, 0)

    for copy in srs:
        copy.wait_recv()
    stot = s_all[here].astype(F32)
    for k in range(level - 1):
        stot = stot + s_rs[k].astype(F32)
    s_n[...] = stot.reshape(NEAR, ring, stot.shape[1])
    sn = [
        go(s_n.at[(a + 1) % NEAR], s_nr.at[0], at(dz=1)),
        go(s_n.at[(a + 3) % NEAR], s_nr.at[1], at(dz=-1)),
        go(s_n.at[(a + 2) % NEAR], s_nr.at[2], at(dz=2)),
    ]

    for copy in rbf:
        copy.wait_recv()
    rb = rb_q[m].astype(F32)
    for k in range(ring - 1):
        rb = rb + rb_f[k].astype(F32)
    wide = jnp.where(pick, rb.reshape(tok, 1, lanes), 0.0).reshape(tok * s8, lanes)
    right_slope = jnp.sum(two_part(tn, wide, nb).reshape(width, s8, depth), axis=1)
    vtot = jnp.concatenate([left_slope, right_slope], axis=1)
    share = width // level
    for k in range(level):
        v_s[k] = vtot[k * share : (k + 1) * share]
    vrs = []
    for o in range(1, level):
        there, device = peer(o)
        vrs.append(go(v_s.at[there], v_rs.at[o - 1], device))

    for copy in sn:
        copy.wait_recv()
    tile = s_n[a] + s_nr[0] + s_nr[1] + s_nr[2]
    for k in range(share):
        s_f[:, k, :] = tile[:, k * 128 : (k + 1) * 128]
    sf = []
    for o in range(1, ring):
        there, device = far(o)
        sf.append(go(s_f.at[there], s_fr.at[o - 1], device))

    for copy in vrs:
        copy.wait_recv()
    vsum = v_s[here]
    for k in range(level - 1):
        vsum = vsum + v_rs[k]
    v_n[...] = vsum
    vn = [go(v_n, v_nr.at[k], at(dz=dz)) for k, dz in enumerate((1, -1, 2))]
    lax.fori_loop(pairs // 4, pairs // 2, make_update, 0)
    for copy in vn:
        copy.wait_recv()
    v_t[...] = v_n[...] + v_nr[0] + v_nr[1] + v_nr[2]
    vf = [go(v_t, v_fr.at[o - 1], far(o)[1]) for o in range(1, ring)]

    lax.fori_loop(pairs // 2, pairs, make_update, 0)
    leave = pltpu.make_async_copy(out, out_away, load_sem.at[8])
    leave.start()

    from_right = two_part(nt, wide, p2r)
    from_even = two_part(nt, lsum, p1e).reshape(pairs, 1, s8, depth)
    from_odd = two_part(nt, lsum, p1o).reshape(pairs, 1, s8, depth)
    from_left = jnp.concatenate([from_even, from_odd], axis=1).reshape(tok, s8, depth)
    scaled = (from_right.reshape(tok, s8, depth) + from_left) * gain[...][None]
    slope[...] = rs * (
        scaled
        - jnp.mean(scaled, axis=-1, keepdims=True)
        - xhat * jnp.mean(scaled * xhat, axis=-1, keepdims=True)
    )

    for copy in sf:
        copy.wait_recv()
    line = s_f[m]
    for k in range(ring - 1):
        line = line + s_fr[k]
    wslope[...] = line

    for copy in vf:
        copy.wait_recv()
    vline = v_t[...]
    for k in range(ring - 1):
        vline = vline + v_fr[k]
    v_f[here] = vline
    vag = [go(v_f.at[here], v_f.at[here], peer(o)[1]) for o in range(1, level)]
    for copy in vag:
        copy.wait_recv()
    for k in range(level):
        part = v_f[k]
        slope1[k * share : (k + 1) * share, :] = part[:, 0:depth]
        slope2[k * share : (k + 1) * share, :] = part[:, depth : 2 * depth]

    leave.wait()
    for copy in started:
        copy.wait_send()


PARTS = 4


def finish(*refs):
    count = (len(refs) - 2) // 3
    sources, targets, held = refs[:count], refs[count : 2 * count], refs[2 * count : 3 * count]
    in_sem, out_sem = refs[-2:]
    moves = []
    for k, (source, target, here) in enumerate(zip(sources, targets, held)):
        if k:
            moves.append((source, here, target))
            continue
        step = source.shape[0] // PARTS
        for n in range(PARTS):
            cut = pl.ds(n * step, step)
            moves.append((source.at[cut], here.at[cut], target.at[cut]))
    loads = [pltpu.make_async_copy(a, b, in_sem.at[n]) for n, (a, b, _) in enumerate(moves)]
    stores = [pltpu.make_async_copy(b, c, out_sem.at[n]) for n, (_, b, c) in enumerate(moves)]
    for copy in loads:
        copy.start()
    for load, store in zip(loads, stores):
        load.wait()
        store.start()
    for copy in stores:
        copy.wait()


def solution(mesh):
    X, Z = mesh.shape["cols"], mesh.shape["rows"] // CORES

    def local(feat, gain, offset, p1, p2, w, bias, cot):
        tok, s8, depth = feat.shape
        width = p1.shape[1]
        share = width // (CORES * X)
        pair_ch = w.shape[1]
        block = cot.shape[1]
        ring, mem, pairs = Z // NEAR, Z // X // NEAR, tok // 2
        lanes, half, seqs = width * s8, 4 * width, s8 * X
        level = CORES * X
        v = pltpu.VMEM
        scratch = [
            v(cot.shape, BF16),
            v(feat.shape, F32),
            v((1, depth), F32),
            v((1, depth), F32),
            v((width, depth), BF16),
            v((width, depth), BF16),
            v(w.shape, BF16),
            v((1, pair_ch), F32),
            v(cot.shape, BF16),
            v(w.shape, F32),
            v((width // 2, half, 2 * pair_ch), BF16),
            v((pairs, X, s8, half), F32),
            v((pairs * seqs * 2, half), BF16),
            v((half, pairs * seqs * 2), BF16),
            v((ring, tok, lanes), BF16),
            v((X, mem, NEAR, CORES, tok, lanes), BF16),
            v((X, lanes, block), BF16),
            v((pairs, X, lanes, 2 * pair_ch), BF16),
            v((pairs, X, lanes, 2 * pair_ch), BF16),
            v((X, mem, NEAR, CORES, tok, lanes), BF16),
            v((X, mem, NEAR, CORES, tok, lanes), F32),
            v((X, mem, NEAR, tok, lanes), BF16),
            v((NEAR, X, mem, tok, lanes), BF16),
            v((X, mem, tok, lanes), F32),
            v((NEAR - 1, X, mem, tok, lanes), BF16),
            v((X, mem, tok, lanes), BF16),
            v((ring, tok, lanes), BF16),
            v((ring - 1, tok, lanes), BF16),
            v((pairs * seqs * 2, half), F32),
            v((pairs, X, s8, half), F32),
            v((X - 1, pairs, s8, half), F32),
            v((level, width, share * pair_ch), BF16),
            v((level - 1, width, share * pair_ch), BF16),
            v((NEAR, ring, share * pair_ch), F32),
            v((NEAR - 1, ring, share * pair_ch), F32),
            v((ring, share, pair_ch), F32),
            v((ring - 1, share, pair_ch), F32),
            v((level, share, 2 * depth), F32),
            v((level - 1, share, 2 * depth), F32),
            v((share, 2 * depth), F32),
            v((NEAR - 1, share, 2 * depth), F32),
            v((share, 2 * depth), F32),
            v((ring - 1, share, 2 * depth), F32),
            v((level, share, 2 * depth), F32),
            pltpu.SemaphoreType.DMA((SEMS,)),
            pltpu.SemaphoreType.DMA((SEMS,)),
            pltpu.SemaphoreType.DMA((9,)),
        ]
        whole = pl.BlockSpec(memory_space=pltpu.VMEM)
        away = pl.BlockSpec(memory_space=pltpu.HBM)
        shapes = tuple(
            jax.ShapeDtypeStruct(dims, kind)
            for dims, kind in (
                (cot.shape, BF16),
                (feat.shape, F32),
                ((share, pair_ch), F32),
                ((width, depth), F32),
                ((width, depth), F32),
            )
        )
        found = pl.pallas_call(
            functools.partial(kernel, X, Z),
            out_shape=shapes,
            in_specs=[away] * 8,
            out_specs=(away,) + (whole,) * 4,
            scratch_shapes=scratch,
            compiler_params=pltpu.CompilerParams(
                collective_id=0, has_side_effects=True, vmem_limit_bytes=VMEM_BYTES
            ),
            name="outer_mean",
        )(feat, gain.reshape(1, -1), offset.reshape(1, -1), p1.T, p2.T, w, bias.reshape(1, -1), cot)
        done = pl.pallas_call(
            finish,
            out_shape=shapes,
            in_specs=[away] * 5,
            out_specs=(away,) * 5,
            scratch_shapes=[v(one.shape, one.dtype) for one in shapes]
            + [pltpu.SemaphoreType.DMA((PARTS + 4,))] * 2,
            compiler_params=pltpu.CompilerParams(vmem_limit_bytes=VMEM_BYTES),
            name="finish",
        )(*found)
        return (*done[:3], done[3].T, done[4].T)

    tokens = P(("groups", "rows"), "cols", None)
    return jax.shard_map(
        local,
        mesh=mesh,
        in_specs=(tokens, P(), P(), P(), P(), P(), P(), tokens),
        out_specs=(tokens, tokens, P(("groups", "rows", "cols"), None), P("groups", None), P("groups", None)),
        check_vma=False,
    )
```

```python
import functools

import jax
import jax.numpy as jnp
from jax import lax
from jax.experimental import pallas as pl
from jax.experimental.pallas import tpu as pltpu
from jax.sharding import PartitionSpec as P

F32 = jnp.float32
BF16 = jnp.bfloat16
NEAR = 4
CORES = 2
SEMS = 128
VMEM_BYTES = 66 * 1000 * 1000


def iota(shape, dim):
    return lax.broadcasted_iota(jnp.int32, shape, dim)


def nn(a, b):
    return jnp.dot(a, b, preferred_element_type=F32)


def nt(a, b):
    return lax.dot_general(a, b, (((1,), (1,)), ((), ())), preferred_element_type=F32)


def tn(a, b):
    return lax.dot_general(a, b, (((0,), (0,)), ((), ())), preferred_element_type=F32)


def two_part(form, a, b):
    high = a.astype(BF16)
    low = (a - high.astype(F32)).astype(BF16)
    return form(high, b) + form(low, b)


def kernel(
    X, Z, feat_in, gain_in, offset_in, p1_in, p2_in, w_in, bias_in, cot_in,
    out_away, slope, wslope, slope1, slope2,
    out, feat, gain, offset, p1, p2, w, bias, cot, wf, wb, lf, lp2, lpt2, ring_r, r_all, rt, t_all, q_all,
    rb_bf, rb_own, rb_d, rb_n, rb_o, rb_r, rb_x, rb_q, rb_f,
    lb_acc, lb, lb_r, s_all, s_rs, s_n, s_nr, s_f, s_fr,
    v_s, v_rs, v_t, v_fr, v_f, send_sem, recv_sem, load_sem,
):
    ring = Z // NEAR
    mem = Z // X // NEAR
    tok = feat.shape[0]
    pairs = tok // 2
    s8 = feat.shape[1]
    width = p1.shape[0]
    lanes = width * s8
    xi = lax.axis_index("cols")
    row = lax.axis_index("rows")
    z, core = row // CORES, row % CORES
    a, m = z % NEAR, z // NEAR
    scale = 1.0 / (s8 * X)

    def at(dx=0, dz=0, other=None):
        k = core if other is None else other
        return {"rows": ((z + dz + Z) % Z) * CORES + k, "cols": (xi + dx) % X}

    used = [0]

    def send(src, dst, device):
        k = used[0]
        used[0] += 1
        copy = pltpu.make_async_remote_copy(
            src_ref=src, dst_ref=dst, send_sem=send_sem.at[k], recv_sem=recv_sem.at[k],
            device_id=device, device_id_type=pl.DeviceIdType.MESH,
        )
        copy.start()
        return copy

    started = []

    def go(src, dst, device):
        copy = send(src, dst, device)
        started.append(copy)
        return copy

    level = CORES * X
    here = xi * CORES + core

    def peer(o):
        there = (here + o) % level
        return there, {"rows": z * CORES + there % CORES, "cols": there // CORES}

    sources = (feat_in, gain_in, offset_in, p2_in, p1_in, w_in, bias_in, cot_in)
    targets = (feat, gain, offset, p2, p1, w, bias, cot)
    loads = [
        pltpu.make_async_copy(source, target, load_sem.at[k])
        for k, (source, target) in enumerate(zip(sources, targets))
    ]
    for copy in loads:
        copy.start()
    steps = (1, -1, 2, -2)
    barrier = pltpu.get_barrier_semaphore()
    for o in range(1, level):
        pl.semaphore_signal(barrier, inc=1, device_id=peer(o)[1], device_id_type=pl.DeviceIdType.MESH)
    for dz in steps:
        pl.semaphore_signal(barrier, inc=1, device_id=at(dz=dz), device_id_type=pl.DeviceIdType.MESH)
    for o in range(1, ring):

        @pl.when(m + o < ring)
        def _(o=o):
            pl.semaphore_signal(
                barrier, inc=1, device_id=at(dz=NEAR * o), device_id_type=pl.DeviceIdType.MESH
            )

    @pl.when(m > 0)
    def _():
        pl.semaphore_signal(barrier, inc=1, device_id=at(dz=-NEAR), device_id_type=pl.DeviceIdType.MESH)


    for copy in loads[:5]:
        copy.wait()
    f = feat[...]
    centred = f - jnp.mean(f, axis=-1, keepdims=True)
    rs = lax.rsqrt(jnp.mean(centred * centred, axis=-1, keepdims=True) + 1e-05)
    xhat = centred * rs
    normed = xhat * gain[...][None] + offset[...][None]
    depth = f.shape[2]
    split = normed.reshape(pairs, 2, s8, depth)
    even = split[:, 0].reshape(pairs * s8, depth).astype(BF16)
    odd = split[:, 1].reshape(pairs * s8, depth).astype(BF16)
    nb = normed.reshape(tok * s8, depth).astype(BF16)

    rep = (iota((width, lanes), 1) // s8 == iota((width, lanes), 0)).astype(BF16)
    p2r = tn(p2[...], rep).astype(BF16)
    half = 2 * 2 * width
    col = iota((width, half), 1)
    same = col % width == iota((width, half), 0)
    p1e = tn(p1[...], (same & ((col // width) % 2 == 0)).astype(BF16)).astype(BF16)
    p1o = tn(p1[...], (same & ((col // width) % 2 == 1)).astype(BF16)).astype(BF16)
    pick = iota((tok, s8, lanes), 1) == iota((tok, s8, lanes), 2) % s8

    right = nn(nb, p2r).reshape(tok, s8, lanes)
    ring_r[m] = jnp.sum(jnp.where(pick, right, 0.0), axis=1).astype(BF16)
    left = (nn(even, p1e) + nn(odd, p1o)).astype(BF16).astype(F32)
    lf[:, xi] = left.reshape(pairs, s8, half)

    wb[...] = jnp.zeros_like(wb)
    loads[5].wait()
    wf[...] = w[...].astype(F32)

    def spread(g, _):
        for d2 in range(2):
            piece = wf[pl.ds(2 * g + d2, width, stride=width), :].astype(BF16)
            for i in range(2):
                at_row = (d2 * 2 + i) * width
                wb[g, at_row : at_row + width, i * 128 : (i + 1) * 128] = piece
        return 0

    lax.fori_loop(0, width // 2, spread, 0)
    pl.semaphore_wait(barrier, level - 1 + len(steps) + m + 1 - m // (ring - 1))

    base = SEMS - 2 * ring

    def remote(k, q, dz):
        return pltpu.make_async_remote_copy(
            src_ref=ring_r.at[q], dst_ref=ring_r.at[q],
            send_sem=send_sem.at[k], recv_sem=recv_sem.at[k],
            device_id=at(dz=dz), device_id_type=pl.DeviceIdType.MESH,
        )

    def down(o):
        return remote(base + o, m, -NEAR * o)

    def up(j):
        return remote(base + ring + j, m - j, NEAR)

    lefts = [go(lf.at[:, xi], lf.at[:, xi], at(dx=dx)) for dx in range(1, X)]

    @pl.when(m < ring - 1)
    def _():
        up(0).start()

    for o in range(ring - 1, 0, -1):

        @pl.when(m >= o)
        def _(o=o):
            down(o).start()

    for copy in lefts:
        copy.wait_recv()

    lane = iota((pairs * X, s8, half), 2)
    lfull = lf[...].reshape(pairs * X, s8, half)
    zero = jnp.zeros_like(lfull)
    both = jnp.concatenate(
        [jnp.where(lane < half // 2, lfull, zero), jnp.where(lane >= half // 2, lfull, zero)], axis=1
    )
    lp2[...] = both.reshape(pairs * X * s8 * 2, half).astype(BF16)
    er, ec = iota((half, half), 0), iota((half, half), 1)
    kept = (er // width) * width + (er % ring) * NEAR + (er % width) // ring
    lpt2[...] = nt((kept == ec).astype(BF16), lp2[...]).astype(BF16)

    def make_t(g, _):
        for u in range(2):
            piece = nn(lp2[...], wb[2 * g + u]).astype(BF16).reshape(pairs, X, 2 * s8, 256)
            at_row = pl.multiple_of((2 * g + u) * 2 * s8, 2 * s8)
            t_all[:, :, pl.ds(at_row, 2 * s8), :] = piece
        return 0

    lax.fori_loop(0, width // 4, make_t, 0)
    loads[6].wait()
    loads[7].wait()

    def pair_of(p):
        return jnp.concatenate([cot[2 * p], cot[2 * p + 1]], axis=-1)

    def make_rb(k, _):
        total = nt(pair_of(0), t_all[0, k])
        for p in range(1, pairs):
            total = total + nt(pair_of(p), t_all[p, k])
        total = (total * scale).reshape(mem, NEAR, CORES, tok, lanes)
        rb_bf[k] = total.astype(BF16)
        rb_own[k] = total
        return 0

    lax.fori_loop(0, X, make_rb, 0)
    rbd = go(rb_bf.at[:, :, :, 1 - core], rb_d, at(other=1 - core))

    for j in range(ring - 1):

        @pl.when(m > j)
        def _(j=j):
            remote(base + ring + j, m - 1 - j, NEAR).wait_recv()

        @pl.when((m > j) & (m < ring - 1))
        def _(j=j):
            up(j + 1).start()

    rbd.wait_recv()
    for k in range(NEAR):
        piece = rb_own[:, :, k, core] + rb_d[:, :, k].astype(F32)
        rb_n[k] = piece.astype(BF16)
    hx = X // 2
    rbn = [
        go(rb_n.at[(a + 1) % NEAR], rb_r.at[0], at(dz=1)),
        go(rb_n.at[(a + 3) % NEAR], rb_r.at[1], at(dz=-1)),
        go(rb_n.at[(a + 2) % NEAR, 0:hx], rb_r.at[2, 0:hx], at(dz=2)),
        go(rb_n.at[(a + 2) % NEAR, hx:X], rb_r.at[2, hx:X], at(dz=-2)),
    ]
    rb_o[...] = rb_own[:, :, a, core] + rb_d[:, :, a].astype(F32)

    for o in range(1, ring):

        @pl.when(m + o < ring)
        def _(o=o):
            down(o).wait_recv()

    rx = [
        go(ring_r.at[pl.ds(((xi + dx) % X) * mem, mem)], r_all.at[xi, :, a, core], at(dx=dx))
        for dx in range(1, X)
    ]
    r_all[xi, :, a, core] = ring_r[pl.ds(xi * mem, mem)]
    partner = at(other=1 - core)

    for copy in rx:
        copy.wait_recv()
    rn = [
        go(r_all.at[:, :, a, core], r_all.at[:, :, a, core], at(dz=1)),
        go(r_all.at[:, :, a, core], r_all.at[:, :, a, core], at(dz=-1)),
        go(r_all.at[0:hx, :, a, core], r_all.at[0:hx, :, a, core], at(dz=2)),
        go(r_all.at[hx:X, :, a, core], r_all.at[hx:X, :, a, core], at(dz=-2)),
    ]

    for copy in rbn:
        copy.wait_recv()
    rb_x[...] = (
        rb_o[...] + rb_r[0].astype(F32) + rb_r[1].astype(F32) + rb_r[2].astype(F32)
    ).astype(BF16)
    rbx = [
        go(rb_x.at[(xi + dx) % X], rb_q.at[pl.ds(xi * mem, mem)], at(dx=dx)) for dx in range(1, X)
    ]
    rb_q[pl.ds(xi * mem, mem)] = rb_x[xi]

    def to_partner(k):
        return go(r_all.at[:, :, k, core], r_all.at[:, :, k, core], partner)

    cores = [to_partner(a)]

    def far(o):
        return (m + o) % ring, at(dz=NEAR * o)

    for copy in rbx:
        copy.wait_recv()
    rbf = []
    for o in range(1, ring):
        there, device = far(o)
        rbf.append(go(rb_q.at[there], rb_f.at[o - 1], device))

    rn[0].wait_recv()
    cores.append(to_partner((a + 3) % NEAR))
    rn[1].wait_recv()
    cores.append(to_partner((a + 1) % NEAR))
    rn[2].wait_recv()
    rn[3].wait_recv()
    cores.append(to_partner((a + 2) % NEAR))
    for copy in cores:
        copy.wait_recv()

    block = mem * NEAR * CORES * tok

    def turn(k, _):
        rt[k] = r_all[k].reshape(block, lanes).T
        return 0

    lax.fori_loop(0, X, turn, 0)

    def make_q(p, _):
        pair = pair_of(p)
        for k in range(X):
            q_all[p, k] = nn(rt[k], pair).astype(BF16)
        return 0

    lax.fori_loop(0, pairs, make_q, 0)

    lb_acc[...] = jnp.zeros_like(lb_acc)

    def of_q(g):
        at_row = pl.multiple_of(g * 2 * s8, 2 * s8)
        return q_all[:, :, pl.ds(at_row, 2 * s8), :].reshape(pairs * X * 2 * s8, 256)

    def make_lb(g, _):
        total = nt(of_q(4 * g), wb[4 * g])
        for u in range(1, 4):
            total = total + nt(of_q(4 * g + u), wb[4 * g + u])
        lb_acc[...] += total
        return 0

    lax.fori_loop(0, width // 8, make_lb, 0)
    acc = lb_acc[...].reshape(pairs * X, 2, s8, half)
    lb[...] = (jnp.where(lane < half // 2, acc[:, 0], acc[:, 1]) * scale).reshape(pairs, X, s8, half)
    lbx = [go(lb.at[:, (xi + dx) % X], lb_r.at[dx - 1], at(dx=dx)) for dx in range(1, X)]

    def make_s(g, _):
        there = (g % X) * CORES + g // X
        for u in range(2):
            found = nn(lpt2[...], of_q(2 * g + u)) * scale
            for d2 in range(2):
                top = d2 * 2 * width
                s_all[there, :, (2 * u + d2) * 128 : (2 * u + d2 + 1) * 128] = (
                    found[top : top + width, 0:128] + found[top + width : top + 2 * width, 128:256]
                ).astype(BF16)
        return 0

    lax.fori_loop(0, width // 4, make_s, 0)
    srs = []
    for o in range(1, level):
        there, device = peer(o)
        srs.append(go(s_all.at[there], s_rs.at[o - 1], device))

    def make_update(p, _):
        total = nn(r_all[0].reshape(block, lanes), t_all[p, 0])
        for k in range(1, X):
            total = total + nn(r_all[k].reshape(block, lanes), t_all[p, k])
        total = total * scale
        out[2 * p] = (total[:, 0:128] + bias[...]).astype(BF16)
        out[2 * p + 1] = (total[:, 128:256] + bias[...]).astype(BF16)
        return 0

    for copy in lbx:
        copy.wait_recv()
    lsum = (lb[:, xi] + lb_r[0] + lb_r[1] + lb_r[2]).reshape(pairs * s8, half)
    f1 = two_part(tn, lsum, even)
    f2 = two_part(tn, lsum, odd)
    left_slope = f1[0:width] + f1[2 * width : 3 * width] + f2[width : 2 * width] + f2[3 * width :]
    for copy in rbf:
        copy.wait_recv()
    rb = rb_q[m].astype(F32)
    for k in range(ring - 1):
        rb = rb + rb_f[k].astype(F32)
    wide = jnp.where(pick, rb.reshape(tok, 1, lanes), 0.0).reshape(tok * s8, lanes)
    right_slope = jnp.sum(two_part(tn, wide, nb).reshape(width, s8, depth), axis=1)
    vtot = jnp.concatenate([left_slope, right_slope], axis=1)
    share = width // level
    for k in range(level):
        v_s[k] = vtot[k * share : (k + 1) * share]
    vrs = []
    for n, dz in enumerate((0, 1, -1, 2)):
        for o in range(level):
            if n or o:
                there = (here + o) % level
                device = at(dz=dz)
                device = {
                    "rows": (device["rows"] // CORES) * CORES + there % CORES,
                    "cols": there // CORES,
                }
                vrs.append(go(v_s.at[there], v_rs.at[n * level + o - 1], device))

    for copy in srs:
        copy.wait_recv()
    stot = s_all[here].astype(F32)
    for k in range(level - 1):
        stot = stot + s_rs[k].astype(F32)
    s_n[...] = stot.reshape(NEAR, ring, stot.shape[1])
    sn = [
        go(s_n.at[(a + 1) % NEAR], s_nr.at[0], at(dz=1)),
        go(s_n.at[(a + 3) % NEAR], s_nr.at[1], at(dz=-1)),
        go(s_n.at[(a + 2) % NEAR], s_nr.at[2], at(dz=2)),
    ]

    for copy in vrs:
        copy.wait_recv()
    v_t[...] = v_s[here] + jnp.sum(v_rs[...], axis=0)
    vf = [go(v_t, v_fr.at[o - 1], far(o)[1]) for o in range(1, ring)]

    for copy in sn:
        copy.wait_recv()
    tile = s_n[a] + s_nr[0] + s_nr[1] + s_nr[2]
    for k in range(share):
        s_f[:, k, :] = tile[:, k * 128 : (k + 1) * 128]
    sf = []
    for o in range(1, ring):
        there, device = far(o)
        sf.append(go(s_f.at[there], s_fr.at[o - 1], device))

    lax.fori_loop(0, pairs, make_update, 0)
    leave = pltpu.make_async_copy(out, out_away, load_sem.at[8])
    leave.start()

    from_right = two_part(nt, wide, p2r)
    from_even = two_part(nt, lsum, p1e).reshape(pairs, 1, s8, depth)
    from_odd = two_part(nt, lsum, p1o).reshape(pairs, 1, s8, depth)
    from_left = jnp.concatenate([from_even, from_odd], axis=1).reshape(tok, s8, depth)
    scaled = (from_right.reshape(tok, s8, depth) + from_left) * gain[...][None]
    slope[...] = rs * (
        scaled
        - jnp.mean(scaled, axis=-1, keepdims=True)
        - xhat * jnp.mean(scaled * xhat, axis=-1, keepdims=True)
    )

    for copy in sf:
        copy.wait_recv()
    line = s_f[m]
    for k in range(ring - 1):
        line = line + s_fr[k]
    wslope[...] = line

    for copy in vf:
        copy.wait_recv()
    vline = v_t[...]
    for k in range(ring - 1):
        vline = vline + v_fr[k]
    v_f[here] = vline
    vag = [go(v_f.at[here], v_f.at[here], peer(o)[1]) for o in range(1, level)]
    for copy in vag:
        copy.wait_recv()
    for k in range(level):
        part = v_f[k]
        slope1[k * share : (k + 1) * share, :] = part[:, 0:depth]
        slope2[k * share : (k + 1) * share, :] = part[:, depth : 2 * depth]

    leave.wait()

    @pl.when(m < ring - 1)
    def _():
        up(0).wait_send()

    for o in range(1, ring):

        @pl.when(m >= o)
        def _(o=o):
            down(o).wait_send()

    for j in range(ring - 1):

        @pl.when((m > j) & (m < ring - 1))
        def _(j=j):
            up(j + 1).wait_send()

    for copy in started:
        copy.wait_send()


PARTS = 4


def finish(*refs):
    count = (len(refs) - 2) // 3
    sources, targets, held = refs[:count], refs[count : 2 * count], refs[2 * count : 3 * count]
    in_sem, out_sem = refs[-2:]
    moves = []
    for k, (source, target, here) in enumerate(zip(sources, targets, held)):
        if k:
            moves.append((source, here, target))
            continue
        step = source.shape[0] // PARTS
        for n in range(PARTS):
            cut = pl.ds(n * step, step)
            moves.append((source.at[cut], here.at[cut], target.at[cut]))
    loads = [pltpu.make_async_copy(a, b, in_sem.at[n]) for n, (a, b, _) in enumerate(moves)]
    stores = [pltpu.make_async_copy(b, c, out_sem.at[n]) for n, (_, b, c) in enumerate(moves)]
    for copy in loads:
        copy.start()
    for load, store in zip(loads, stores):
        load.wait()
        store.start()
    for copy in stores:
        copy.wait()


def solution(mesh):
    X, Z = mesh.shape["cols"], mesh.shape["rows"] // CORES

    def local(feat, gain, offset, p1, p2, w, bias, cot):
        tok, s8, depth = feat.shape
        width = p1.shape[1]
        share = width // (CORES * X)
        pair_ch = w.shape[1]
        block = cot.shape[1]
        ring, mem, pairs = Z // NEAR, Z // X // NEAR, tok // 2
        lanes, half, seqs = width * s8, 4 * width, s8 * X
        level = CORES * X
        v = pltpu.VMEM
        scratch = [
            v(cot.shape, BF16),
            v(feat.shape, F32),
            v((1, depth), F32),
            v((1, depth), F32),
            v((width, depth), BF16),
            v((width, depth), BF16),
            v(w.shape, BF16),
            v((1, pair_ch), F32),
            v(cot.shape, BF16),
            v(w.shape, F32),
            v((width // 2, half, 2 * pair_ch), BF16),
            v((pairs, X, s8, half), F32),
            v((pairs * seqs * 2, half), BF16),
            v((half, pairs * seqs * 2), BF16),
            v((ring, tok, lanes), BF16),
            v((X, mem, NEAR, CORES, tok, lanes), BF16),
            v((X, lanes, block), BF16),
            v((pairs, X, lanes, 2 * pair_ch), BF16),
            v((pairs, X, lanes, 2 * pair_ch), BF16),
            v((X, mem, NEAR, CORES, tok, lanes), BF16),
            v((X, mem, NEAR, CORES, tok, lanes), F32),
            v((X, mem, NEAR, tok, lanes), BF16),
            v((NEAR, X, mem, tok, lanes), BF16),
            v((X, mem, tok, lanes), F32),
            v((NEAR - 1, X, mem, tok, lanes), BF16),
            v((X, mem, tok, lanes), BF16),
            v((ring, tok, lanes), BF16),
            v((ring - 1, tok, lanes), BF16),
            v((pairs * seqs * 2, half), F32),
            v((pairs, X, s8, half), F32),
            v((X - 1, pairs, s8, half), F32),
            v((level, width, share * pair_ch), BF16),
            v((level - 1, width, share * pair_ch), BF16),
            v((NEAR, ring, share * pair_ch), F32),
            v((NEAR - 1, ring, share * pair_ch), F32),
            v((ring, share, pair_ch), F32),
            v((ring - 1, share, pair_ch), F32),
            v((level, share, 2 * depth), F32),
            v((NEAR * level - 1, share, 2 * depth), F32),
            v((share, 2 * depth), F32),
            v((ring - 1, share, 2 * depth), F32),
            v((level, share, 2 * depth), F32),
            pltpu.SemaphoreType.DMA((SEMS,)),
            pltpu.SemaphoreType.DMA((SEMS,)),
            pltpu.SemaphoreType.DMA((9,)),
        ]
        whole = pl.BlockSpec(memory_space=pltpu.VMEM)
        away = pl.BlockSpec(memory_space=pltpu.HBM)
        shapes = tuple(
            jax.ShapeDtypeStruct(dims, kind)
            for dims, kind in (
                (cot.shape, BF16),
                (feat.shape, F32),
                ((share, pair_ch), F32),
                ((width, depth), F32),
                ((width, depth), F32),
            )
        )
        found = pl.pallas_call(
            functools.partial(kernel, X, Z),
            out_shape=shapes,
            in_specs=[away] * 8,
            out_specs=(away,) + (whole,) * 4,
            scratch_shapes=scratch,
            compiler_params=pltpu.CompilerParams(
                collective_id=0, has_side_effects=True, vmem_limit_bytes=VMEM_BYTES
            ),
            name="outer_mean",
        )(feat, gain.reshape(1, -1), offset.reshape(1, -1), p1.T, p2.T, w, bias.reshape(1, -1), cot)
        done = pl.pallas_call(
            finish,
            out_shape=shapes,
            in_specs=[away] * 5,
            out_specs=(away,) * 5,
            scratch_shapes=[v(one.shape, one.dtype) for one in shapes]
            + [pltpu.SemaphoreType.DMA((PARTS + 4,))] * 2,
            compiler_params=pltpu.CompilerParams(vmem_limit_bytes=VMEM_BYTES),
            name="finish",
        )(*found)
        return (*done[:3], done[3].T, done[4].T)

    tokens = P(("groups", "rows"), "cols", None)
    return jax.shard_map(
        local,
        mesh=mesh,
        in_specs=(tokens, P(), P(), P(), P(), P(), P(), tokens),
        out_specs=(tokens, tokens, P(("groups", "rows", "cols"), None), P("groups", None), P("groups", None)),
        check_vma=False,
    )
```

```python
import functools

import jax
import jax.numpy as jnp
from jax import lax
from jax.experimental import pallas as pl
from jax.experimental.pallas import tpu as pltpu
from jax.sharding import PartitionSpec as P

F32 = jnp.float32
BF16 = jnp.bfloat16
NEAR = 4
CORES = 2
SEMS = 128
VMEM_BYTES = 66 * 1000 * 1000


def iota(shape, dim):
    return lax.broadcasted_iota(jnp.int32, shape, dim)


def nn(a, b):
    return jnp.dot(a, b, preferred_element_type=F32)


def nt(a, b):
    return lax.dot_general(a, b, (((1,), (1,)), ((), ())), preferred_element_type=F32)


def tn(a, b):
    return lax.dot_general(a, b, (((0,), (0,)), ((), ())), preferred_element_type=F32)


def two_part(form, a, b):
    high = a.astype(BF16)
    low = (a - high.astype(F32)).astype(BF16)
    return form(high, b) + form(low, b)


def kernel(
    X, Z, feat_in, gain_in, offset_in, p1_in, p2_in, w_in, bias_in, cot_in,
    out_away, slope, wslope, slope1, slope2,
    out, feat, gain, offset, p1, p2, w, bias, cot, wf, wb, lf, lp2, lpt2, ring_r, r_all, rt, t_all, q_all,
    rb_bf, rb_own, rb_d, rb_n, rb_o, rb_r, rb_x, rb_q, rb_f,
    lb_acc, lb, lb_r, s_all, s_rs, s_n, s_nr, sv, sv_r,
    v_s, v_rs, v_f, send_sem, recv_sem, load_sem,
):
    ring = Z // NEAR
    mem = Z // X // NEAR
    tok = feat.shape[0]
    pairs = tok // 2
    s8 = feat.shape[1]
    width = p1.shape[0]
    lanes = width * s8
    xi = lax.axis_index("cols")
    row = lax.axis_index("rows")
    z, core = row // CORES, row % CORES
    a, m = z % NEAR, z // NEAR
    scale = 1.0 / (s8 * X)

    def at(dx=0, dz=0, other=None):
        k = core if other is None else other
        return {"rows": ((z + dz + Z) % Z) * CORES + k, "cols": (xi + dx) % X}

    used = [0]

    def send(src, dst, device):
        k = used[0]
        used[0] += 1
        copy = pltpu.make_async_remote_copy(
            src_ref=src, dst_ref=dst, send_sem=send_sem.at[k], recv_sem=recv_sem.at[k],
            device_id=device, device_id_type=pl.DeviceIdType.MESH,
        )
        copy.start()
        return copy

    started = []

    def go(src, dst, device):
        copy = send(src, dst, device)
        started.append(copy)
        return copy

    level = CORES * X
    here = xi * CORES + core

    def peer(o):
        there = (here + o) % level
        return there, {"rows": z * CORES + there % CORES, "cols": there // CORES}

    sources = (feat_in, gain_in, offset_in, p2_in, p1_in, w_in, bias_in, cot_in)
    targets = (feat, gain, offset, p2, p1, w, bias, cot)
    loads = [
        pltpu.make_async_copy(source, target, load_sem.at[k])
        for k, (source, target) in enumerate(zip(sources, targets))
    ]
    for copy in loads:
        copy.start()
    steps = (1, -1, 2, -2, NEAR, -NEAR)
    barrier = pltpu.get_barrier_semaphore()
    for o in range(1, level):
        pl.semaphore_signal(barrier, inc=1, device_id=peer(o)[1], device_id_type=pl.DeviceIdType.MESH)
    for dz in steps:
        pl.semaphore_signal(barrier, inc=1, device_id=at(dz=dz), device_id_type=pl.DeviceIdType.MESH)

    for copy in loads[:5]:
        copy.wait()
    f = feat[...]
    centred = f - jnp.mean(f, axis=-1, keepdims=True)
    rs = lax.rsqrt(jnp.mean(centred * centred, axis=-1, keepdims=True) + 1e-05)
    xhat = centred * rs
    normed = xhat * gain[...][None] + offset[...][None]
    depth = f.shape[2]
    split = normed.reshape(pairs, 2, s8, depth)
    even = split[:, 0].reshape(pairs * s8, depth).astype(BF16)
    odd = split[:, 1].reshape(pairs * s8, depth).astype(BF16)
    nb = normed.reshape(tok * s8, depth).astype(BF16)

    rep = (iota((width, lanes), 1) // s8 == iota((width, lanes), 0)).astype(BF16)
    p2r = tn(p2[...], rep).astype(BF16)
    half = 2 * 2 * width
    col = iota((width, half), 1)
    same = col % width == iota((width, half), 0)
    p1e = tn(p1[...], (same & ((col // width) % 2 == 0)).astype(BF16)).astype(BF16)
    p1o = tn(p1[...], (same & ((col // width) % 2 == 1)).astype(BF16)).astype(BF16)
    pick = iota((tok, s8, lanes), 1) == iota((tok, s8, lanes), 2) % s8

    right = nn(nb, p2r).reshape(tok, s8, lanes)
    ring_r[m] = jnp.sum(jnp.where(pick, right, 0.0), axis=1).astype(BF16)
    left = (nn(even, p1e) + nn(odd, p1o)).astype(BF16).astype(F32)
    lf[:, xi] = left.reshape(pairs, s8, half)

    wb[...] = jnp.zeros_like(wb)
    loads[5].wait()
    wf[...] = w[...].astype(F32)

    def spread(g, _):
        for d2 in range(2):
            piece = wf[pl.ds(2 * g + d2, width, stride=width), :].astype(BF16)
            for i in range(2):
                at_row = (d2 * 2 + i) * width
                wb[g, at_row : at_row + width, i * 128 : (i + 1) * 128] = piece
        return 0

    lax.fori_loop(0, width // 2, spread, 0)
    pl.semaphore_wait(barrier, level - 1 + len(steps))

    def ring_up(buf, t):
        q = (m - t + 1 + ring) % ring
        return go(buf.at[q], buf.at[q], at(dz=NEAR))

    def ring_down(buf, t):
        q = (m + t - 1) % ring
        return go(buf.at[q], buf.at[q], at(dz=-NEAR))

    ups, downs = ring // 2, ring // 2 - 1

    lefts = [go(lf.at[:, xi], lf.at[:, xi], at(dx=dx)) for dx in range(1, X)]
    up, down = ring_up(ring_r, 1), ring_down(ring_r, 1)
    for copy in lefts:
        copy.wait_recv()

    lane = iota((pairs * X, s8, half), 2)
    lfull = lf[...].reshape(pairs * X, s8, half)
    zero = jnp.zeros_like(lfull)
    both = jnp.concatenate(
        [jnp.where(lane < half // 2, lfull, zero), jnp.where(lane >= half // 2, lfull, zero)], axis=1
    )
    lp2[...] = both.reshape(pairs * X * s8 * 2, half).astype(BF16)
    er, ec = iota((half, half), 0), iota((half, half), 1)
    kept = (er // width) * width + (er % ring) * NEAR + (er % width) // ring
    lpt2[...] = nt((kept == ec).astype(BF16), lp2[...]).astype(BF16)

    def make_t(g, _):
        for u in range(2):
            piece = nn(lp2[...], wb[2 * g + u]).astype(BF16).reshape(pairs, X, 2 * s8, 256)
            at_row = pl.multiple_of((2 * g + u) * 2 * s8, 2 * s8)
            t_all[:, :, pl.ds(at_row, 2 * s8), :] = piece
        return 0

    lax.fori_loop(0, width // 8, make_t, 0)

    up.wait_recv()
    up2 = ring_up(ring_r, 2)
    down.wait_recv()
    down2 = ring_down(ring_r, 2)
    lax.fori_loop(width // 8, width // 4, make_t, 0)
    loads[6].wait()
    loads[7].wait()

    def pair_of(p):
        return jnp.concatenate([cot[2 * p], cot[2 * p + 1]], axis=-1)

    def make_rb(k, _):
        total = nt(pair_of(0), t_all[0, k])
        for p in range(1, pairs):
            total = total + nt(pair_of(p), t_all[p, k])
        total = (total * scale).reshape(mem, NEAR, CORES, tok, lanes)
        rb_bf[k] = total.astype(BF16)
        rb_own[k] = total
        return 0

    lax.fori_loop(0, X, make_rb, 0)
    rbd = go(rb_bf.at[:, :, :, 1 - core], rb_d, at(other=1 - core))

    up2.wait_recv()
    up3 = ring_up(ring_r, 3)
    down2.wait_recv()
    down3 = ring_down(ring_r, 3)

    rbd.wait_recv()
    for k in range(NEAR):
        piece = rb_own[:, :, k, core] + rb_d[:, :, k].astype(F32)
        rb_n[k] = piece.astype(BF16)
    hx = X // 2
    rbn = [
        go(rb_n.at[(a + 1) % NEAR], rb_r.at[0], at(dz=1)),
        go(rb_n.at[(a + 3) % NEAR], rb_r.at[1], at(dz=-1)),
        go(rb_n.at[(a + 2) % NEAR, 0:hx], rb_r.at[2, 0:hx], at(dz=2)),
        go(rb_n.at[(a + 2) % NEAR, hx:X], rb_r.at[2, hx:X], at(dz=-2)),
    ]
    rb_o[...] = rb_own[:, :, a, core] + rb_d[:, :, a].astype(F32)

    up3.wait_recv()
    up4 = ring_up(ring_r, 4)

    for copy in rbn:
        copy.wait_recv()
    rb_x[...] = (
        rb_o[...] + rb_r[0].astype(F32) + rb_r[1].astype(F32) + rb_r[2].astype(F32)
    ).astype(BF16)
    rbx = [
        go(rb_x.at[(xi + dx) % X], rb_q.at[pl.ds(xi * mem, mem)], at(dx=dx)) for dx in range(1, X)
    ]
    rb_q[pl.ds(xi * mem, mem)] = rb_x[xi]

    down3.wait_recv()
    up4.wait_recv()
    rx = [
        go(ring_r.at[pl.ds(((xi + dx) % X) * mem, mem)], r_all.at[xi, :, a, core], at(dx=dx))
        for dx in range(1, X)
    ]
    r_all[xi, :, a, core] = ring_r[pl.ds(xi * mem, mem)]
    partner = at(other=1 - core)

    for copy in rx:
        copy.wait_recv()
    rn = [
        go(r_all.at[:, :, a, core], r_all.at[:, :, a, core], at(dz=1)),
        go(r_all.at[:, :, a, core], r_all.at[:, :, a, core], at(dz=-1)),
        go(r_all.at[0:hx, :, a, core], r_all.at[0:hx, :, a, core], at(dz=2)),
        go(r_all.at[hx:X, :, a, core], r_all.at[hx:X, :, a, core], at(dz=-2)),
    ]

    def to_partner(k):
        return go(r_all.at[:, :, k, core], r_all.at[:, :, k, core], partner)

    cores = [to_partner(a)]

    def far(o):
        return (m + o) % ring, at(dz=NEAR * o)

    for copy in rbx:
        copy.wait_recv()
    rbf = []
    for o in sorted(range(1, ring), key=lambda o: -min(o, ring - o)):
        there, device = far(o)
        rbf.append(go(rb_q.at[there], rb_f.at[o - 1], device))

    rn[0].wait_recv()
    cores.append(to_partner((a + 3) % NEAR))
    rn[1].wait_recv()
    cores.append(to_partner((a + 1) % NEAR))
    rn[2].wait_recv()
    rn[3].wait_recv()
    cores.append(to_partner((a + 2) % NEAR))
    for copy in cores:
        copy.wait_recv()

    block = mem * NEAR * CORES * tok

    def turn(k, _):
        rt[k] = r_all[k].reshape(block, lanes).T
        return 0

    lax.fori_loop(0, X, turn, 0)

    def make_q(p, _):
        pair = pair_of(p)
        for k in range(X):
            q_all[p, k] = nn(rt[k], pair).astype(BF16)
        return 0

    lax.fori_loop(0, pairs, make_q, 0)

    lb_acc[...] = jnp.zeros_like(lb_acc)

    def of_q(g):
        at_row = pl.multiple_of(g * 2 * s8, 2 * s8)
        return q_all[:, :, pl.ds(at_row, 2 * s8), :].reshape(pairs * X * 2 * s8, 256)

    def make_lb(g, _):
        total = nt(of_q(4 * g), wb[4 * g])
        for u in range(1, 4):
            total = total + nt(of_q(4 * g + u), wb[4 * g + u])
        lb_acc[...] += total
        return 0

    lax.fori_loop(0, width // 8, make_lb, 0)
    acc = lb_acc[...].reshape(pairs * X, 2, s8, half)
    lb[...] = (jnp.where(lane < half // 2, acc[:, 0], acc[:, 1]) * scale).reshape(pairs, X, s8, half)
    lbx = [go(lb.at[:, (xi + dx) % X], lb_r.at[dx - 1], at(dx=dx)) for dx in range(1, X)]

    def make_s(g, _):
        there = (g % X) * CORES + g // X
        for u in range(2):
            found = nn(lpt2[...], of_q(2 * g + u)) * scale
            for d2 in range(2):
                top = d2 * 2 * width
                s_all[there, :, (2 * u + d2) * 128 : (2 * u + d2 + 1) * 128] = (
                    found[top : top + width, 0:128] + found[top + width : top + 2 * width, 128:256]
                ).astype(BF16)
        return 0

    lax.fori_loop(0, width // 4, make_s, 0)
    srs = []
    for o in range(1, level):
        there, device = peer(o)
        srs.append(go(s_all.at[there], s_rs.at[o - 1], device))

    def make_update(p, _):
        total = nn(r_all[0].reshape(block, lanes), t_all[p, 0])
        for k in range(1, X):
            total = total + nn(r_all[k].reshape(block, lanes), t_all[p, k])
        total = total * scale
        out[2 * p] = (total[:, 0:128] + bias[...]).astype(BF16)
        out[2 * p + 1] = (total[:, 128:256] + bias[...]).astype(BF16)
        return 0

    for copy in lbx:
        copy.wait_recv()
    lsum = (lb[:, xi] + lb_r[0] + lb_r[1] + lb_r[2]).reshape(pairs * s8, half)
    f1 = two_part(tn, lsum, even)
    f2 = two_part(tn, lsum, odd)
    left_slope = f1[0:width] + f1[2 * width : 3 * width] + f2[width : 2 * width] + f2[3 * width :]
    for copy in rbf:
        copy.wait_recv()
    rb = rb_q[m].astype(F32)
    for k in range(ring - 1):
        rb = rb + rb_f[k].astype(F32)
    wide = jnp.where(pick, rb.reshape(tok, 1, lanes), 0.0).reshape(tok * s8, lanes)
    right_slope = jnp.sum(two_part(tn, wide, nb).reshape(width, s8, depth), axis=1)
    vtot = jnp.concatenate([left_slope, right_slope], axis=1)
    share = width // level
    for k in range(level):
        v_s[k] = vtot[k * share : (k + 1) * share]
    vrs = []
    for n, dz in enumerate((0, 1, -1, 2)):
        for o in range(level):
            if n or o:
                there = (here + o) % level
                device = at(dz=dz)
                device = {
                    "rows": (device["rows"] // CORES) * CORES + there % CORES,
                    "cols": there // CORES,
                }
                vrs.append(go(v_s.at[there], v_rs.at[n * level + o - 1], device))

    for copy in srs:
        copy.wait_recv()
    stot = s_all[here].astype(F32)
    for k in range(level - 1):
        stot = stot + s_rs[k].astype(F32)
    s_n[...] = stot.reshape(NEAR, ring, stot.shape[1])
    sn = [
        go(s_n.at[(a + 1) % NEAR], s_nr.at[0], at(dz=1)),
        go(s_n.at[(a + 3) % NEAR], s_nr.at[1], at(dz=-1)),
        go(s_n.at[(a + 2) % NEAR], s_nr.at[2], at(dz=2)),
    ]

    for copy in vrs:
        copy.wait_recv()
    both_here = v_s[here] + jnp.sum(v_rs[...], axis=0)
    for k in range(ring):
        sv[k, share : 2 * share] = both_here

    for copy in sn:
        copy.wait_recv()
    tile = s_n[a] + s_nr[0] + s_nr[1] + s_nr[2]
    for k in range(share):
        sv[:, k, :] = tile[:, k * 128 : (k + 1) * 128]
    svf = []
    for o in sorted(range(1, ring), key=lambda o: -min(o, ring - o)):
        there, device = far(o)
        svf.append(go(sv.at[there], sv_r.at[o - 1], device))

    lax.fori_loop(0, pairs, make_update, 0)
    leave = pltpu.make_async_copy(out, out_away, load_sem.at[8])
    leave.start()

    from_right = two_part(nt, wide, p2r)
    from_even = two_part(nt, lsum, p1e).reshape(pairs, 1, s8, depth)
    from_odd = two_part(nt, lsum, p1o).reshape(pairs, 1, s8, depth)
    from_left = jnp.concatenate([from_even, from_odd], axis=1).reshape(tok, s8, depth)
    scaled = (from_right.reshape(tok, s8, depth) + from_left) * gain[...][None]
    slope[...] = rs * (
        scaled
        - jnp.mean(scaled, axis=-1, keepdims=True)
        - xhat * jnp.mean(scaled * xhat, axis=-1, keepdims=True)
    )

    for copy in svf:
        copy.wait_recv()
    total = sv[m] + jnp.sum(sv_r[...], axis=0)
    v_f[here] = total[share:]
    vag = [go(v_f.at[here], v_f.at[here], peer(o)[1]) for o in range(1, level)]
    wslope[...] = total[:share]
    for copy in vag:
        copy.wait_recv()
    for k in range(level):
        part = v_f[k]
        slope1[k * share : (k + 1) * share, :] = part[:, 0:depth]
        slope2[k * share : (k + 1) * share, :] = part[:, depth : 2 * depth]

    leave.wait()
    for copy in started:
        copy.wait_send()


PARTS = 4


def finish(*refs):
    count = (len(refs) - 2) // 3
    sources, targets, held = refs[:count], refs[count : 2 * count], refs[2 * count : 3 * count]
    in_sem, out_sem = refs[-2:]
    moves = []
    for k, (source, target, here) in enumerate(zip(sources, targets, held)):
        if k:
            moves.append((source, here, target))
            continue
        step = source.shape[0] // PARTS
        for n in range(PARTS):
            cut = pl.ds(n * step, step)
            moves.append((source.at[cut], here.at[cut], target.at[cut]))
    loads = [pltpu.make_async_copy(a, b, in_sem.at[n]) for n, (a, b, _) in enumerate(moves)]
    stores = [pltpu.make_async_copy(b, c, out_sem.at[n]) for n, (_, b, c) in enumerate(moves)]
    for copy in loads:
        copy.start()
    for load, store in zip(loads, stores):
        load.wait()
        store.start()
    for copy in stores:
        copy.wait()


def solution(mesh):
    X, Z = mesh.shape["cols"], mesh.shape["rows"] // CORES

    def local(feat, gain, offset, p1, p2, w, bias, cot):
        tok, s8, depth = feat.shape
        width = p1.shape[1]
        share = width // (CORES * X)
        pair_ch = w.shape[1]
        block = cot.shape[1]
        ring, mem, pairs = Z // NEAR, Z // X // NEAR, tok // 2
        lanes, half, seqs = width * s8, 4 * width, s8 * X
        level = CORES * X
        v = pltpu.VMEM
        scratch = [
            v(cot.shape, BF16),
            v(feat.shape, F32),
            v((1, depth), F32),
            v((1, depth), F32),
            v((width, depth), BF16),
            v((width, depth), BF16),
            v(w.shape, BF16),
            v((1, pair_ch), F32),
            v(cot.shape, BF16),
            v(w.shape, F32),
            v((width // 2, half, 2 * pair_ch), BF16),
            v((pairs, X, s8, half), F32),
            v((pairs * seqs * 2, half), BF16),
            v((half, pairs * seqs * 2), BF16),
            v((ring, tok, lanes), BF16),
            v((X, mem, NEAR, CORES, tok, lanes), BF16),
            v((X, lanes, block), BF16),
            v((pairs, X, lanes, 2 * pair_ch), BF16),
            v((pairs, X, lanes, 2 * pair_ch), BF16),
            v((X, mem, NEAR, CORES, tok, lanes), BF16),
            v((X, mem, NEAR, CORES, tok, lanes), F32),
            v((X, mem, NEAR, tok, lanes), BF16),
            v((NEAR, X, mem, tok, lanes), BF16),
            v((X, mem, tok, lanes), F32),
            v((NEAR - 1, X, mem, tok, lanes), BF16),
            v((X, mem, tok, lanes), BF16),
            v((ring, tok, lanes), BF16),
            v((ring - 1, tok, lanes), BF16),
            v((pairs * seqs * 2, half), F32),
            v((pairs, X, s8, half), F32),
            v((X - 1, pairs, s8, half), F32),
            v((level, width, share * pair_ch), BF16),
            v((level - 1, width, share * pair_ch), BF16),
            v((NEAR, ring, share * pair_ch), F32),
            v((NEAR - 1, ring, share * pair_ch), F32),
            v((ring, 2 * share, pair_ch), F32),
            v((ring - 1, 2 * share, pair_ch), F32),
            v((level, share, 2 * depth), F32),
            v((NEAR * level - 1, share, 2 * depth), F32),
            v((level, share, 2 * depth), F32),
            pltpu.SemaphoreType.DMA((SEMS,)),
            pltpu.SemaphoreType.DMA((SEMS,)),
            pltpu.SemaphoreType.DMA((9,)),
        ]
        whole = pl.BlockSpec(memory_space=pltpu.VMEM)
        away = pl.BlockSpec(memory_space=pltpu.HBM)
        shapes = tuple(
            jax.ShapeDtypeStruct(dims, kind)
            for dims, kind in (
                (cot.shape, BF16),
                (feat.shape, F32),
                ((share, pair_ch), F32),
                ((width, depth), F32),
                ((width, depth), F32),
            )
        )
        found = pl.pallas_call(
            functools.partial(kernel, X, Z),
            out_shape=shapes,
            in_specs=[away] * 8,
            out_specs=(away,) + (whole,) * 4,
            scratch_shapes=scratch,
            compiler_params=pltpu.CompilerParams(
                collective_id=0, has_side_effects=True, vmem_limit_bytes=VMEM_BYTES
            ),
            name="outer_mean",
        )(feat, gain.reshape(1, -1), offset.reshape(1, -1), p1.T, p2.T, w, bias.reshape(1, -1), cot)
        done = pl.pallas_call(
            finish,
            out_shape=shapes,
            in_specs=[away] * 5,
            out_specs=(away,) * 5,
            scratch_shapes=[v(one.shape, one.dtype) for one in shapes]
            + [pltpu.SemaphoreType.DMA((PARTS + 4,))] * 2,
            compiler_params=pltpu.CompilerParams(vmem_limit_bytes=VMEM_BYTES),
            name="finish",
        )(*found)
        return (*done[:3], done[3].T, done[4].T)

    tokens = P(("groups", "rows"), "cols", None)
    return jax.shard_map(
        local,
        mesh=mesh,
        in_specs=(tokens, P(), P(), P(), P(), P(), P(), tokens),
        out_specs=(tokens, tokens, P(("groups", "rows", "cols"), None), P("groups", None), P("groups", None)),
        check_vma=False,
    )
```

```python
import functools

import jax
import jax.numpy as jnp
from jax import lax
from jax.experimental import pallas as pl
from jax.experimental.pallas import tpu as pltpu
from jax.sharding import PartitionSpec as P

F32 = jnp.float32
BF16 = jnp.bfloat16
NEAR = 4
CORES = 2
SEMS = 128
VMEM_BYTES = 66 * 1000 * 1000


def iota(shape, dim):
    return lax.broadcasted_iota(jnp.int32, shape, dim)


def nn(a, b):
    return jnp.dot(a, b, preferred_element_type=F32)


def nt(a, b):
    return lax.dot_general(a, b, (((1,), (1,)), ((), ())), preferred_element_type=F32)


def tn(a, b):
    return lax.dot_general(a, b, (((0,), (0,)), ((), ())), preferred_element_type=F32)


def two_part(form, a, b):
    high = a.astype(BF16)
    low = (a - high.astype(F32)).astype(BF16)
    return form(high, b) + form(low, b)


def kernel(
    X, Z, feat_in, gain_in, offset_in, p1_in, p2_in, w_in, bias_in, cot_in,
    out_away, slope, wslope, slope1, slope2,
    out, feat, gain, offset, p1, p2, w, bias, cot, wf, wb, lf, lp2, lpt2, ring_r, r_all, rt, t_all, q_all,
    rb_bf, rb_own, rb_d, rb_n, rb_o, rb_r, rb_x, rb_q, rb_f,
    lb_acc, lb, lb_r, s_all, s_rs, s_n, s_nr, sv, sv_r,
    v_s, v_rs, v_f, send_sem, recv_sem, load_sem,
):
    ring = Z // NEAR
    mem = Z // X // NEAR
    tok = feat.shape[0]
    pairs = tok // 2
    s8 = feat.shape[1]
    width = p1.shape[0]
    lanes = width * s8
    xi = lax.axis_index("cols")
    row = lax.axis_index("rows")
    z, core = row // CORES, row % CORES
    a, m = z % NEAR, z // NEAR
    scale = 1.0 / (s8 * X)

    def at(dx=0, dz=0, other=None):
        k = core if other is None else other
        return {"rows": ((z + dz + Z) % Z) * CORES + k, "cols": (xi + dx) % X}

    used = [0]

    def send(src, dst, device):
        k = used[0]
        used[0] += 1
        copy = pltpu.make_async_remote_copy(
            src_ref=src, dst_ref=dst, send_sem=send_sem.at[k], recv_sem=recv_sem.at[k],
            device_id=device, device_id_type=pl.DeviceIdType.MESH,
        )
        copy.start()
        return copy

    started = []

    def go(src, dst, device):
        copy = send(src, dst, device)
        started.append(copy)
        return copy

    level = CORES * X
    here = xi * CORES + core

    def peer(o):
        there = (here + o) % level
        return there, {"rows": z * CORES + there % CORES, "cols": there // CORES}

    sources = (feat_in, gain_in, offset_in, p2_in, p1_in, w_in, bias_in, cot_in)
    targets = (feat, gain, offset, p2, p1, w, bias, cot)
    loads = [
        pltpu.make_async_copy(source, target, load_sem.at[k])
        for k, (source, target) in enumerate(zip(sources, targets))
    ]
    for copy in loads:
        copy.start()
    steps = (1, -1, 2, -2, NEAR, -NEAR)
    barrier = pltpu.get_barrier_semaphore()
    for o in range(1, level):
        pl.semaphore_signal(barrier, inc=1, device_id=peer(o)[1], device_id_type=pl.DeviceIdType.MESH)
    for dz in steps:
        pl.semaphore_signal(barrier, inc=1, device_id=at(dz=dz), device_id_type=pl.DeviceIdType.MESH)

    for copy in loads[:5]:
        copy.wait()
    f = feat[...]
    centred = f - jnp.mean(f, axis=-1, keepdims=True)
    rs = lax.rsqrt(jnp.mean(centred * centred, axis=-1, keepdims=True) + 1e-05)
    xhat = centred * rs
    normed = xhat * gain[...][None] + offset[...][None]
    depth = f.shape[2]
    split = normed.reshape(pairs, 2, s8, depth)
    even = split[:, 0].reshape(pairs * s8, depth).astype(BF16)
    odd = split[:, 1].reshape(pairs * s8, depth).astype(BF16)
    nb = normed.reshape(tok * s8, depth).astype(BF16)

    rep = (iota((width, lanes), 1) // s8 == iota((width, lanes), 0)).astype(BF16)
    p2r = tn(p2[...], rep).astype(BF16)
    half = 2 * 2 * width
    col = iota((width, half), 1)
    same = col % width == iota((width, half), 0)
    p1e = tn(p1[...], (same & ((col // width) % 2 == 0)).astype(BF16)).astype(BF16)
    p1o = tn(p1[...], (same & ((col // width) % 2 == 1)).astype(BF16)).astype(BF16)
    pick = iota((tok, s8, lanes), 1) == iota((tok, s8, lanes), 2) % s8

    right = nn(nb, p2r).reshape(tok, s8, lanes)
    ring_r[m] = jnp.sum(jnp.where(pick, right, 0.0), axis=1).astype(BF16)
    left = (nn(even, p1e) + nn(odd, p1o)).astype(BF16).astype(F32)
    lf[:, xi] = left.reshape(pairs, s8, half)

    wb[...] = jnp.zeros_like(wb)
    loads[5].wait()
    wf[...] = w[...].astype(F32)

    def spread(g, _):
        for d2 in range(2):
            piece = wf[pl.ds(2 * g + d2, width, stride=width), :].astype(BF16)
            for i in range(2):
                at_row = (d2 * 2 + i) * width
                wb[g, at_row : at_row + width, i * 128 : (i + 1) * 128] = piece
        return 0

    lax.fori_loop(0, width // 2, spread, 0)
    pl.semaphore_wait(barrier, level - 1 + len(steps))

    def ring_up(buf, t):
        q = (m - t + 1 + ring) % ring
        return go(buf.at[q], buf.at[q], at(dz=NEAR))

    def ring_down(buf, t):
        q = (m + t - 1) % ring
        return go(buf.at[q], buf.at[q], at(dz=-NEAR))

    ups, downs = ring // 2, ring // 2 - 1

    lefts = [go(lf.at[:, xi], lf.at[:, xi], at(dx=dx)) for dx in range(1, X)]
    up, down = ring_up(ring_r, 1), ring_down(ring_r, 1)
    up.wait_recv()
    up2 = ring_up(ring_r, 2)
    down.wait_recv()
    down2 = ring_down(ring_r, 2)
    for copy in lefts:
        copy.wait_recv()

    lane = iota((pairs * X, s8, half), 2)
    lfull = lf[...].reshape(pairs * X, s8, half)
    zero = jnp.zeros_like(lfull)
    both = jnp.concatenate(
        [jnp.where(lane < half // 2, lfull, zero), jnp.where(lane >= half // 2, lfull, zero)], axis=1
    )
    lp2[...] = both.reshape(pairs * X * s8 * 2, half).astype(BF16)
    er, ec = iota((half, half), 0), iota((half, half), 1)
    kept = (er // width) * width + (er % ring) * NEAR + (er % width) // ring
    lpt2[...] = nt((kept == ec).astype(BF16), lp2[...]).astype(BF16)

    def make_t(g, _):
        for u in range(2):
            piece = nn(lp2[...], wb[2 * g + u]).astype(BF16).reshape(pairs, X, 2 * s8, 256)
            at_row = pl.multiple_of((2 * g + u) * 2 * s8, 2 * s8)
            t_all[:, :, pl.ds(at_row, 2 * s8), :] = piece
        return 0

    lax.fori_loop(0, width // 4, make_t, 0)
    loads[6].wait()
    loads[7].wait()

    def pair_of(p):
        return jnp.concatenate([cot[2 * p], cot[2 * p + 1]], axis=-1)

    def make_rb(k, _):
        total = nt(pair_of(0), t_all[0, k])
        for p in range(1, pairs):
            total = total + nt(pair_of(p), t_all[p, k])
        total = (total * scale).reshape(mem, NEAR, CORES, tok, lanes)
        rb_bf[k] = total.astype(BF16)
        rb_own[k] = total
        return 0

    lax.fori_loop(0, X, make_rb, 0)
    rbd = go(rb_bf.at[:, :, :, 1 - core], rb_d, at(other=1 - core))

    up2.wait_recv()
    up3 = ring_up(ring_r, 3)
    down2.wait_recv()
    down3 = ring_down(ring_r, 3)

    rbd.wait_recv()
    for k in range(NEAR):
        piece = rb_own[:, :, k, core] + rb_d[:, :, k].astype(F32)
        rb_n[k] = piece.astype(BF16)
    hx = X // 2
    rbn = [
        go(rb_n.at[(a + 1) % NEAR], rb_r.at[0], at(dz=1)),
        go(rb_n.at[(a + 3) % NEAR], rb_r.at[1], at(dz=-1)),
        go(rb_n.at[(a + 2) % NEAR, 0:hx], rb_r.at[2, 0:hx], at(dz=2)),
        go(rb_n.at[(a + 2) % NEAR, hx:X], rb_r.at[2, hx:X], at(dz=-2)),
    ]
    rb_o[...] = rb_own[:, :, a, core] + rb_d[:, :, a].astype(F32)

    up3.wait_recv()
    up4 = ring_up(ring_r, 4)

    for copy in rbn:
        copy.wait_recv()
    rb_x[...] = (
        rb_o[...] + rb_r[0].astype(F32) + rb_r[1].astype(F32) + rb_r[2].astype(F32)
    ).astype(BF16)
    rbx = [
        go(rb_x.at[(xi + dx) % X], rb_q.at[pl.ds(xi * mem, mem)], at(dx=dx)) for dx in range(1, X)
    ]
    rb_q[pl.ds(xi * mem, mem)] = rb_x[xi]

    down3.wait_recv()
    up4.wait_recv()
    rx = [
        go(ring_r.at[pl.ds(((xi + dx) % X) * mem, mem)], r_all.at[xi, :, a, core], at(dx=dx))
        for dx in range(1, X)
    ]
    r_all[xi, :, a, core] = ring_r[pl.ds(xi * mem, mem)]
    partner = at(other=1 - core)

    for copy in rx:
        copy.wait_recv()
    rn = [
        go(r_all.at[:, :, a, core], r_all.at[:, :, a, core], at(dz=1)),
        go(r_all.at[:, :, a, core], r_all.at[:, :, a, core], at(dz=-1)),
        go(r_all.at[0:hx, :, a, core], r_all.at[0:hx, :, a, core], at(dz=2)),
        go(r_all.at[hx:X, :, a, core], r_all.at[hx:X, :, a, core], at(dz=-2)),
    ]

    def to_partner(k):
        return go(r_all.at[:, :, k, core], r_all.at[:, :, k, core], partner)

    cores = [to_partner(a)]

    def far(o):
        return (m + o) % ring, at(dz=NEAR * o)

    for copy in rbx:
        copy.wait_recv()
    rbf = []
    for o in sorted(range(1, ring), key=lambda o: -min(o, ring - o)):
        there, device = far(o)
        rbf.append(go(rb_q.at[there], rb_f.at[o - 1], device))

    rn[0].wait_recv()
    cores.append(to_partner((a + 3) % NEAR))
    rn[1].wait_recv()
    cores.append(to_partner((a + 1) % NEAR))
    rn[2].wait_recv()
    rn[3].wait_recv()
    cores.append(to_partner((a + 2) % NEAR))
    for copy in cores:
        copy.wait_recv()

    block = mem * NEAR * CORES * tok

    def turn(k, _):
        rt[k] = r_all[k].reshape(block, lanes).T
        return 0

    lax.fori_loop(0, X, turn, 0)

    def make_q(p, _):
        pair = pair_of(p)
        for k in range(X):
            q_all[p, k] = nn(rt[k], pair).astype(BF16)
        return 0

    lax.fori_loop(0, pairs, make_q, 0)

    lb_acc[...] = jnp.zeros_like(lb_acc)

    def of_q(g):
        at_row = pl.multiple_of(g * 2 * s8, 2 * s8)
        return q_all[:, :, pl.ds(at_row, 2 * s8), :].reshape(pairs * X * 2 * s8, 256)

    def make_lb(g, _):
        total = nt(of_q(4 * g), wb[4 * g])
        for u in range(1, 4):
            total = total + nt(of_q(4 * g + u), wb[4 * g + u])
        lb_acc[...] += total
        return 0

    lax.fori_loop(0, width // 8, make_lb, 0)
    acc = lb_acc[...].reshape(pairs * X, 2, s8, half)
    lb[...] = (jnp.where(lane < half // 2, acc[:, 0], acc[:, 1]) * scale).reshape(pairs, X, s8, half)
    lbx = [go(lb.at[:, (xi + dx) % X], lb_r.at[dx - 1], at(dx=dx)) for dx in range(1, X)]

    srs = []
    for o in range(1, level + 1):
        there, device = peer(o)
        g = (there % CORES) * X + there // CORES
        for u in range(2):
            found = nn(lpt2[...], of_q(2 * g + u)) * scale
            for d2 in range(2):
                top = d2 * 2 * width
                s_all[there, :, (2 * u + d2) * 128 : (2 * u + d2 + 1) * 128] = (
                    found[top : top + width, 0:128] + found[top + width : top + 2 * width, 128:256]
                ).astype(BF16)
        if o < level:
            srs.append(go(s_all.at[there], s_rs.at[o - 1], device))

    def make_update(p, _):
        total = nn(r_all[0].reshape(block, lanes), t_all[p, 0])
        for k in range(1, X):
            total = total + nn(r_all[k].reshape(block, lanes), t_all[p, k])
        total = total * scale
        out[2 * p] = (total[:, 0:128] + bias[...]).astype(BF16)
        out[2 * p + 1] = (total[:, 128:256] + bias[...]).astype(BF16)
        return 0

    for copy in lbx:
        copy.wait_recv()
    lsum = (lb[:, xi] + lb_r[0] + lb_r[1] + lb_r[2]).reshape(pairs * s8, half)
    f1 = two_part(tn, lsum, even)
    f2 = two_part(tn, lsum, odd)
    left_slope = f1[0:width] + f1[2 * width : 3 * width] + f2[width : 2 * width] + f2[3 * width :]
    for copy in rbf:
        copy.wait_recv()
    rb = rb_q[m].astype(F32)
    for k in range(ring - 1):
        rb = rb + rb_f[k].astype(F32)
    wide = jnp.where(pick, rb.reshape(tok, 1, lanes), 0.0).reshape(tok * s8, lanes)
    right_slope = jnp.sum(two_part(tn, wide, nb).reshape(width, s8, depth), axis=1)
    vtot = jnp.concatenate([left_slope, right_slope], axis=1)
    share = width // level
    for k in range(level):
        v_s[k] = vtot[k * share : (k + 1) * share]
    vrs = []
    for n, dz in enumerate((0, 1, -1, 2)):
        for o in range(level):
            if n or o:
                there = (here + o) % level
                device = at(dz=dz)
                device = {
                    "rows": (device["rows"] // CORES) * CORES + there % CORES,
                    "cols": there // CORES,
                }
                vrs.append(go(v_s.at[there], v_rs.at[n * level + o - 1], device))

    for copy in srs:
        copy.wait_recv()
    stot = s_all[here].astype(F32)
    for k in range(level - 1):
        stot = stot + s_rs[k].astype(F32)
    s_n[...] = stot.reshape(NEAR, ring, stot.shape[1])
    sn = [
        go(s_n.at[(a + 1) % NEAR], s_nr.at[0], at(dz=1)),
        go(s_n.at[(a + 3) % NEAR], s_nr.at[1], at(dz=-1)),
        go(s_n.at[(a + 2) % NEAR], s_nr.at[2], at(dz=2)),
    ]

    for copy in vrs:
        copy.wait_recv()
    both_here = v_s[here] + jnp.sum(v_rs[...], axis=0)
    for k in range(ring):
        sv[k, share : 2 * share] = both_here

    for copy in sn:
        copy.wait_recv()
    tile = s_n[a] + s_nr[0] + s_nr[1] + s_nr[2]
    for k in range(share):
        sv[:, k, :] = tile[:, k * 128 : (k + 1) * 128]
    svf = []
    for o in sorted(range(1, ring), key=lambda o: -min(o, ring - o)):
        there, device = far(o)
        svf.append(go(sv.at[there], sv_r.at[o - 1], device))

    lax.fori_loop(0, pairs, make_update, 0)
    leave = pltpu.make_async_copy(out, out_away, load_sem.at[8])
    leave.start()

    from_right = two_part(nt, wide, p2r)
    from_even = two_part(nt, lsum, p1e).reshape(pairs, 1, s8, depth)
    from_odd = two_part(nt, lsum, p1o).reshape(pairs, 1, s8, depth)
    from_left = jnp.concatenate([from_even, from_odd], axis=1).reshape(tok, s8, depth)
    scaled = (from_right.reshape(tok, s8, depth) + from_left) * gain[...][None]
    slope[...] = rs * (
        scaled
        - jnp.mean(scaled, axis=-1, keepdims=True)
        - xhat * jnp.mean(scaled * xhat, axis=-1, keepdims=True)
    )

    for copy in svf:
        copy.wait_recv()
    total = sv[m] + jnp.sum(sv_r[...], axis=0)
    v_f[here] = total[share:]
    vag = [go(v_f.at[here], v_f.at[here], peer(o)[1]) for o in range(1, level)]
    wslope[...] = total[:share]
    for copy in vag:
        copy.wait_recv()
    for k in range(level):
        part = v_f[k]
        slope1[k * share : (k + 1) * share, :] = part[:, 0:depth]
        slope2[k * share : (k + 1) * share, :] = part[:, depth : 2 * depth]

    leave.wait()
    for copy in started:
        copy.wait_send()


PARTS = 4


def finish(*refs):
    count = (len(refs) - 2) // 3
    sources, targets, held = refs[:count], refs[count : 2 * count], refs[2 * count : 3 * count]
    in_sem, out_sem = refs[-2:]
    moves = []
    for k, (source, target, here) in enumerate(zip(sources, targets, held)):
        if k:
            moves.append((source, here, target))
            continue
        step = source.shape[0] // PARTS
        for n in range(PARTS):
            cut = pl.ds(n * step, step)
            moves.append((source.at[cut], here.at[cut], target.at[cut]))
    loads = [pltpu.make_async_copy(a, b, in_sem.at[n]) for n, (a, b, _) in enumerate(moves)]
    stores = [pltpu.make_async_copy(b, c, out_sem.at[n]) for n, (_, b, c) in enumerate(moves)]
    for copy in loads:
        copy.start()
    for load, store in zip(loads, stores):
        load.wait()
        store.start()
    for copy in stores:
        copy.wait()


def solution(mesh):
    X, Z = mesh.shape["cols"], mesh.shape["rows"] // CORES

    def local(feat, gain, offset, p1, p2, w, bias, cot):
        tok, s8, depth = feat.shape
        width = p1.shape[1]
        share = width // (CORES * X)
        pair_ch = w.shape[1]
        block = cot.shape[1]
        ring, mem, pairs = Z // NEAR, Z // X // NEAR, tok // 2
        lanes, half, seqs = width * s8, 4 * width, s8 * X
        level = CORES * X
        v = pltpu.VMEM
        scratch = [
            v(cot.shape, BF16),
            v(feat.shape, F32),
            v((1, depth), F32),
            v((1, depth), F32),
            v((width, depth), BF16),
            v((width, depth), BF16),
            v(w.shape, BF16),
            v((1, pair_ch), F32),
            v(cot.shape, BF16),
            v(w.shape, F32),
            v((width // 2, half, 2 * pair_ch), BF16),
            v((pairs, X, s8, half), F32),
            v((pairs * seqs * 2, half), BF16),
            v((half, pairs * seqs * 2), BF16),
            v((ring, tok, lanes), BF16),
            v((X, mem, NEAR, CORES, tok, lanes), BF16),
            v((X, lanes, block), BF16),
            v((pairs, X, lanes, 2 * pair_ch), BF16),
            v((pairs, X, lanes, 2 * pair_ch), BF16),
            v((X, mem, NEAR, CORES, tok, lanes), BF16),
            v((X, mem, NEAR, CORES, tok, lanes), F32),
            v((X, mem, NEAR, tok, lanes), BF16),
            v((NEAR, X, mem, tok, lanes), BF16),
            v((X, mem, tok, lanes), F32),
            v((NEAR - 1, X, mem, tok, lanes), BF16),
            v((X, mem, tok, lanes), BF16),
            v((ring, tok, lanes), BF16),
            v((ring - 1, tok, lanes), BF16),
            v((pairs * seqs * 2, half), F32),
            v((pairs, X, s8, half), F32),
            v((X - 1, pairs, s8, half), F32),
            v((level, width, share * pair_ch), BF16),
            v((level - 1, width, share * pair_ch), BF16),
            v((NEAR, ring, share * pair_ch), F32),
            v((NEAR - 1, ring, share * pair_ch), F32),
            v((ring, 2 * share, pair_ch), F32),
            v((ring - 1, 2 * share, pair_ch), F32),
            v((level, share, 2 * depth), F32),
            v((NEAR * level - 1, share, 2 * depth), F32),
            v((level, share, 2 * depth), F32),
            pltpu.SemaphoreType.DMA((SEMS,)),
            pltpu.SemaphoreType.DMA((SEMS,)),
            pltpu.SemaphoreType.DMA((9,)),
        ]
        whole = pl.BlockSpec(memory_space=pltpu.VMEM)
        away = pl.BlockSpec(memory_space=pltpu.HBM)
        shapes = tuple(
            jax.ShapeDtypeStruct(dims, kind)
            for dims, kind in (
                (cot.shape, BF16),
                (feat.shape, F32),
                ((share, pair_ch), F32),
                ((width, depth), F32),
                ((width, depth), F32),
            )
        )
        found = pl.pallas_call(
            functools.partial(kernel, X, Z),
            out_shape=shapes,
            in_specs=[away] * 8,
            out_specs=(away,) + (whole,) * 4,
            scratch_shapes=scratch,
            compiler_params=pltpu.CompilerParams(
                collective_id=0, has_side_effects=True, vmem_limit_bytes=VMEM_BYTES
            ),
            name="outer_mean",
        )(feat, gain.reshape(1, -1), offset.reshape(1, -1), p1.T, p2.T, w, bias.reshape(1, -1), cot)
        done = pl.pallas_call(
            finish,
            out_shape=shapes,
            in_specs=[away] * 5,
            out_specs=(away,) * 5,
            scratch_shapes=[v(one.shape, one.dtype) for one in shapes]
            + [pltpu.SemaphoreType.DMA((PARTS + 4,))] * 2,
            compiler_params=pltpu.CompilerParams(vmem_limit_bytes=VMEM_BYTES),
            name="finish",
        )(*found)
        return (*done[:3], done[3].T, done[4].T)

    tokens = P(("groups", "rows"), "cols", None)
    return jax.shard_map(
        local,
        mesh=mesh,
        in_specs=(tokens, P(), P(), P(), P(), P(), P(), tokens),
        out_specs=(tokens, tokens, P(("groups", "rows", "cols"), None), P("groups", None), P("groups", None)),
        check_vma=False,
    )
```
